32 devices in a mesh: gx: 2 (over x), gy: 4 (over y, core), gz: 4 (over z).
Axes of the slice: x: 2, y: 2, z: 4, core: 2. Of those that a mesh axis runs over, the one named last changes fastest.
Arguments:
- rhs: float32 [8, 8, 2, 16, 512], P(None, None, 'gx', 'gy', 'gz'), as said below
- blocks: bfloat16 [7, 8, 8, 2, 16, 512], P(None, None, None, 'gx', 'gy', 'gz'), as said below
Outputs:
- basis: float32 [4, 8, 8, 2, 16, 512], P(None, None, None, 'gx', 'gy', 'gz')
- hess: float32 [4, 8, 3, 8], replicated
Inputs may be any that keep to these rules, and one draw needn't show every extreme that they name: `rhs`: each cell's value is a random draw times a positive scale that varies smoothly over the grid. The operator couples each cell only to itself and its six face neighbours; its blocks are full and the block Krylov spaces keep full rank.
All inputs are finite; a program needn't handle non-finite values.
Results may differ from the reference program's by a relative error of at most 0.001.
Values sent between devices are 32-bit elements; how exact they have to be, the bound alone decides.
A program may use at most 64 MiB of HBM per device.

```python
import jax
import jax.numpy as jnp
from jax import lax

BLOCK = 8
RHS = 8
ITERS = 3
NX = 2
NY = 16
NZ = 512


def draw_rhs(key, part):
    shape = (BLOCK, RHS, NX, NY, NZ)
    values = jax.random.normal(key, shape, jnp.float32)
    pos_x = jnp.arange(NX, dtype=jnp.float32)[:, None, None] / NX
    pos_y = jnp.arange(NY, dtype=jnp.float32)[None, :, None] / NY
    pos_z = jnp.arange(NZ, dtype=jnp.float32)[None, None, :] / NZ
    rising = 3.0 ** pos_z * 2.0 ** pos_x * 2.0 ** pos_y
    return values * rising[None, None]


def draw_blocks(key, part):
    key_noise = jax.random.fold_in(key, 11)
    key_center = jax.random.fold_in(key, 12)
    key_flow = jax.random.fold_in(key, 13)
    shape = (7, BLOCK, BLOCK, NX, NY, NZ)
    noise = jax.random.normal(key_noise, shape, jnp.float32)
    center = jax.random.uniform(key_center, (NX, NY, NZ), jnp.float32, 0.0, 1.0)
    flow = jax.random.uniform(key_flow, (3, NX, NY, NZ), jnp.float32, -1.0, 1.0)
    eye = jnp.eye(BLOCK, dtype=jnp.float32)[:, :, None, None, None]
    parts = [(0.8 + 0.4 * center)[None, None] * eye + 0.06 * noise[0]]
    for k in range(1, 7):
        axis_number = (k - 1) // 2
        sign = 1.0 if k % 2 == 1 else -1.0
        weight = -(0.125 + 0.06 * sign * flow[axis_number])
        parts.append(weight[None, None] * eye + 0.02 * noise[k])
    return jnp.stack(parts).astype(jnp.bfloat16)


def setup_inputs(seed: int = 0) -> dict:
    arg_keys = jax.random.split(jax.random.key(seed), 3)
    rhs = draw_rhs(jax.random.fold_in(arg_keys[2], 71), 0)
    blocks = draw_blocks(jax.random.fold_in(arg_keys[2], 71), 0)
    return {"rhs": rhs, "blocks": blocks}


HIGH = lax.Precision.HIGHEST

def operate(field, blocks):
    padded = jnp.pad(field, ((0, 0), (0, 0), (1, 1), (1, 1), (1, 1)))
    views = [padded[:, :, 1:-1, 1:-1, 1:-1], padded[:, :, 2:, 1:-1, 1:-1], padded[:, :, :-2, 1:-1, 1:-1], padded[:, :, 1:-1, 2:, 1:-1], padded[:, :, 1:-1, :-2, 1:-1], padded[:, :, 1:-1, 1:-1, 2:], padded[:, :, 1:-1, 1:-1, :-2]]
    total = jnp.zeros(field.shape, jnp.float32)
    for k in range(7):
        for j in range(field.shape[0]):
            column = blocks[k, :, j].astype(jnp.float32)
            total = total + column[:, None] * views[k][j][None]
    return total

def pair(first, second):
    return jnp.einsum('arxyz,asxyz->rs', first, second, precision=HIGH)

def mix(field, matrix):
    return jnp.einsum('asxyz,sr->arxyz', field, matrix, precision=HIGH)

def normalizer(gram, eye):
    lower = jnp.linalg.cholesky(gram)
    inverse = lax.linalg.triangular_solve(lower, eye, left_side=True, lower=True)
    return (inverse.T, lower.T)

def reference(rhs, blocks):
    eye = jnp.eye(RHS, dtype=jnp.float32)
    scale, upper = normalizer(pair(rhs, rhs), eye)
    basis = [mix(rhs, scale)]
    hess = jnp.zeros((ITERS + 1, RHS, ITERS, RHS), jnp.float32)
    for step in range(ITERS):
        image = operate(basis[step], blocks)
        coeffs = [pair(vector, image) for vector in basis]
        gram = pair(image, image)
        rest = image
        for vector, coeff in zip(basis, coeffs):
            gram = gram - jnp.dot(coeff.T, coeff, precision=HIGH)
            rest = rest - mix(vector, coeff)
        scale, upper = normalizer(gram, eye)
        basis.append(mix(rest, scale))
        for index, coeff in enumerate(coeffs):
            hess = hess.at[index, :, step, :].set(coeff)
        hess = hess.at[step + 1, :, step, :].set(upper)
    return (jnp.stack(basis), hess)
```

```python
import functools

import jax
import jax.numpy as jnp
from jax import lax
from jax.experimental import pallas as pl
from jax.experimental.pallas import tpu as pltpu
from jax.sharding import PartitionSpec as P

ITERS = 3
F32 = jnp.float32
HIGH = lax.Precision.HIGHEST
AXES = ("gx", "gy", "gz")
MESH = pl.DeviceIdType.MESH


def dot_nt(a, b):
    return lax.dot_general(a, b, (((1,), (1,)), ((), ())), precision=HIGH, preferred_element_type=F32)


def dot_nn(a, b):
    return lax.dot_general(a, b, (((1,), (0,)), ((), ())), precision=HIGH, preferred_element_type=F32)


def tile_iota():
    row = lax.broadcasted_iota(jnp.int32, (8, 128), 0)
    lane = lax.broadcasted_iota(jnp.int32, (8, 128), 1)
    return row, lane


def empty():
    return jnp.zeros((8, 128), F32)


def pad_rows(pieces):
    return jnp.concatenate(pieces + [empty()] * (16 - len(pieces)), axis=0)


def spread(ref, index, r):
    return jnp.broadcast_to(ref[index + (pl.ds(r, 1), slice(None))], (8, 128))


def column(m, c):
    return jnp.broadcast_to(m[:, c:c + 1], (8, 128))


def cholesky(s, aug, base, row, lane):
    cols = [column(s, c) for c in range(8)]
    low = empty()
    for k in range(8):
        piv = jnp.broadcast_to(cols[k][k:k + 1], (8, 128))
        rs = lax.rsqrt(piv)
        rs = rs * (1.5 - 0.5 * piv * rs * rs)
        lk = jnp.where(row >= k, cols[k] * rs, 0.0)
        low = low + jnp.where(lane == base + k, lk, 0.0)
        arow = jnp.broadcast_to(aug[k:k + 1], (8, 128)) * rs
        aug = jnp.where(row == k, arow, aug - jnp.where(row > k, lk, 0.0) * arow)
        for c in range(k + 1, 8):
            cols[c] = cols[c] - lk * jnp.broadcast_to(lk[c:c + 1], (8, 128))
    return low, aug


def krylov(
    mesh_sizes, nb, nr, ly, lz,
    rhs_hbm, blk_hbm, q_ref, p3, small,
    rv, bv, cf, vp, p1, p2, xb, xg, zs, zr, zp, loc, aa, ab, ac,
    x_send, x_recv, y_send, y_recv, z_send, z_recv, a_send, a_recv, in_sem, known,
):
    nx, ny, nz = mesh_sizes
    ndev = nx * ny * nz
    gx, gy, gz = (lax.axis_index(a) for a in AXES)
    me = (gx * ny + gy) * nz + gz
    cells = ndev * ly * lz
    row, lane = tile_iota()
    barrier = pltpu.get_barrier_semaphore()

    in_rhs = pltpu.make_async_copy(rhs_hbm, rv, in_sem.at[7])
    in_rhs.start()
    terms = [0, 3, 4, 5, 6, 1, 2]
    in_blk = [pltpu.make_async_copy(blk_hbm.at[k], bv.at[k], in_sem.at[k]) for k in range(7)]
    for k in terms:
        in_blk[k].start()

    def wrapped(at, d, size):
        t = at + d
        return jnp.where(t >= size, t - size, t)

    def greet(sem, axis):
        size, at = {"gx": (nx, gx), "gy": (ny, gy), "gz": (nz, gz)}[axis]
        if size <= 8:
            for d in range(1, size):
                pl.semaphore_signal(sem, inc=1, device_id={axis: wrapped(at, d, size)}, device_id_type=MESH)
        else:
            def body(d, c):
                pl.semaphore_signal(sem, inc=1, device_id={axis: lax.rem(at + d, size)}, device_id_type=MESH)
                return c
            lax.fori_loop(1, size, body, 0)

    for axis in AXES[::-1]:
        greet(barrier, axis)

    if nx == 1:
        x_sides = []
    elif nx == 2:
        x_sides = [(1 + gx, None, 1 - gx)]
    else:
        x_sides = [(1, gx < nx - 1, gx + 1), (2, gx > 0, gx - 1)]

    def when(cond, fn):
        if cond is None:
            fn()
        else:
            pl.when(cond)(fn)

    def remote(src, dst, ssem, rsem, dev):
        return pltpu.make_async_remote_copy(
            src_ref=src, dst_ref=dst, send_sem=ssem, recv_sem=rsem, device_id=dev, device_id_type=MESH)

    def x_copy(n, side, y):
        opposite = side if nx == 2 else 1 - side
        return remote(vp.at[n, 1 + y], xb.at[n, opposite, y], x_send.at[n, side, y],
                      x_recv.at[n, opposite, y], {"gx": x_sides[side][2]})

    def x_arrived(n, side, y):
        remote(vp.at[n, 1 + y], xb.at[n, side, y], x_send.at[n, side, y],
               x_recv.at[n, side, y], {"gx": x_sides[side][2]}).wait_recv()

    def y_copy(n, side):
        if side == 0:
            return remote(vp.at[n, ly], vp.at[n, 0], y_send.at[n, 0], y_recv.at[n, 0], {"gy": gy + 1})
        return remote(vp.at[n, 1], vp.at[n, ly + 1], y_send.at[n, 1], y_recv.at[n, 1], {"gy": gy - 1})

    def z_copy(n, side, y):
        target = gz - 1 if side == 0 else gz + 1
        return remote(zs.at[n, y], zr.at[n, side, y], z_send.at[n, side, y], z_recv.at[n, side, y], {"gz": target})

    y_to = (gy < ny - 1, gy > 0)
    y_from = (gy > 0, gy < ny - 1)
    z_to = (gz > 0, gz < nz - 1)
    z_from = (gz < nz - 1, gz > 0)

    for side in range(2):
        @pl.when(jnp.logical_not(y_from[side]))
        def _():
            for n in range(ITERS):
                vp[n, 0 if side == 0 else ly + 1] = jnp.zeros((nb * 8, 128), F32)

        @pl.when(jnp.logical_not(z_from[side]))
        def _():
            for n in range(ITERS):
                zr[n, side] = jnp.zeros((ly, 8, 128), F32)

    if nx > 2:
        for side in range(2):
            @pl.when(jnp.logical_not(x_sides[side][1]))
            def _():
                for n in range(ITERS):
                    xb[n, side] = jnp.zeros((ly, nb * 8, 128), F32)

    def send_x(n, y):
        for side, entry in enumerate(x_sides):
            when(entry[1], lambda: x_copy(n, side, y).start())

    def send_yz(n, y):
        if y == ly - 1:
            pl.when(y_to[0])(lambda: y_copy(n, 0).start())
        if y == 0:
            pl.when(y_to[1])(lambda: y_copy(n, 1).start())
        edge = empty()
        for a in range(nb):
            v = vp[n, 1 + y, a * 8:(a + 1) * 8]
            edge = jnp.where(lane // 2 == a, pltpu.roll(v, 2 * a + 1, 1), edge)
        zs[n, y] = edge
        for side in range(2):
            pl.when(z_to[side])(lambda: z_copy(n, side, y).start())

    order = [0] + ([ly - 1] if ly > 1 else []) + list(range(1, ly - 1))

    in_rhs.wait()
    for y in order:
        for a in range(nb):
            vp[0, 1 + y, a * 8:(a + 1) * 8] = rv[pl.ds(a * nr * ly + y, 8, stride=ly), :]
    pl.semaphore_wait(barrier, nx + ny + nz - 3)
    for y in order:
        send_x(0, y)
    greet(known.at[0], "gy")
    for y in order:
        send_yz(0, y)

    def convert(k, total):
        def body(i, total):
            rows = bv[k, i].astype(F32)
            cf[k, i] = rows
            for r in range(0, nb * ly, 8):
                total = total + jnp.abs(rows[r:r + 8])
            return total
        return lax.fori_loop(0, nb, body, total)

    total_abs = empty()
    for k in terms:
        in_blk[k].wait()
        total_abs = convert(k, total_abs)
    trace = jnp.zeros((ly, 128), F32)
    for i in range(nb):
        trace = trace + cf[0, i, i * ly:(i + 1) * ly]

    views = [(vp, (0,), 1), (p1, (), 0), (p2, (), 1), (p3, (), 0)]

    def tile(i, y, a):
        ref, index, off = views[i]
        return ref[index + (off + y, pl.ds(pl.multiple_of(a * 8, 8), 8), slice(None))]

    def tile_row(i, y, r):
        ref, index, off = views[i]
        return spread(ref, index + (off + y,), r)

    def gram_row(n, y, acc):
        def body(a, acc):
            p = tile(n, y, a)
            return tuple(acc[i * 8 + s] + p * tile_row(i, y, a * 8 + s)
                         for i in range(n + 1) for s in range(8))
        return lax.fori_loop(0, nb, body, acc)

    def gram_zero(n):
        return tuple(empty() for _ in range(8 * (n + 1)))

    def gram_end(acc, width):
        d = empty()
        for k, part in enumerate(acc):
            d = jnp.where(lane % width == k, jnp.sum(part, axis=1, keepdims=True), d)
        return d

    def gram(n):
        acc = gram_zero(n)
        for y in range(ly):
            acc = gram_row(n, y, acc)
        return acc

    def pack32(d):
        d = jnp.where(lane // 32 == row % 4, d, 0.0)
        return [jnp.sum(d[0:4], axis=0, keepdims=True), jnp.sum(d[4:8], axis=0, keepdims=True)]

    def pack16(d):
        d = jnp.where(lane // 16 == row, d, 0.0)
        return [jnp.sum(d, axis=0, keepdims=True)]

    def unpack32(t0, t1):
        z = jnp.where(row < 4, t0, t1)
        out = z
        for g in range(1, 4):
            out = jnp.where(row % 4 == g, pltpu.roll(z, 128 - 32 * g, 1), out)
        return out

    def unpack16(t):
        z = jnp.broadcast_to(t, (8, 128))
        out = z
        for g in range(1, 8):
            out = jnp.where(row == g, pltpu.roll(z, 128 - 16 * g, 1), out)
        return out

    def far(i, n):
        return min(i, n - i)

    offsets = [(dx, dy, dz) for dx in range(nx) for dy in range(ny) for dz in range(nz) if dx or dy or dz]
    offsets.sort(key=lambda o: -(far(o[0], nx) + far(o[1], ny) + far(o[2], nz)))

    def ar_start(buf, m, rows):
        for r, v in enumerate(rows):
            buf[me, r:r + 1] = v
        if ndev <= 64:
            xs = [wrapped(gx, d, nx) for d in range(nx)]
            ys = [wrapped(gy, d, ny) for d in range(ny)]
            zs_ = [wrapped(gz, d, nz) for d in range(nz)]
            for dx, dy, dz in offsets:
                remote(buf.at[me], buf.at[me], a_send.at[m], a_recv.at[m], (xs[dx], ys[dy], zs_[dz])).start()
        else:
            def body(d, c):
                t = lax.rem(me + d, ndev)
                remote(buf.at[me], buf.at[me], a_send.at[m], a_recv.at[m],
                       (t // (ny * nz), (t // nz) % ny, t % nz)).start()
                return c
            lax.fori_loop(1, ndev, body, 0)

    def ar_wait(buf, sem):
        pltpu.make_async_copy(buf.at[0:ndev - 1], buf.at[0:ndev - 1], sem).wait()

    def ar_done(buf, m):
        ar_wait(buf, a_recv.at[m])
        return jnp.sum(buf[...], axis=0)

    lane_sum = lambda x: jnp.sum(x, axis=1, keepdims=True)
    pl.semaphore_wait(known.at[0], ny - 1)
    greet(known.at[1], "gx")
    d0 = gram_end(gram(0), 32)
    d0 = d0 + jnp.where(lane % 32 == 8, jnp.where(row < ly, lane_sum(jnp.concatenate(
        [trace, jnp.zeros((8 - ly, 128), F32)], axis=0)), 0.0), 0.0)
    d0 = d0 + jnp.where(lane % 32 == 9, lane_sum(total_abs), 0.0)
    pl.semaphore_wait(known.at[1], nx - 1)
    ar_start(aa, 0, pack32(d0))

    def halos(n):
        for side in range(2):
            @pl.when(z_from[side])
            def _():
                for y in range(ly):
                    z_copy(n, side, y).wait_recv()
            pl.when(y_from[side])(lambda: y_copy(n, side).wait_recv())

    def local_rows(n, field, off, edges):
        for y in order:
            plus, minus = edges(y)
            for j in range(nb):
                v = field(off + y, j)
                zp[y, 0, j * 8:(j + 1) * 8] = jnp.where(
                    lane == lz - 1, pltpu.roll(plus, lz - 2 - 2 * j, 1), pltpu.roll(v, lz - 1, 1))
                zp[y, 1, j * 8:(j + 1) * 8] = jnp.where(
                    lane == 0, pltpu.roll(minus, lz - 2 * j, 1) if j else minus, pltpu.roll(v, 1, 1))
        for y in order:
            def body(j, acc):
                at = pl.ds(pl.multiple_of(j * 8, 8), 8)
                values = [field(off + y, j), field(off + y + 1, j), field(off + y - 1, j), zp[y, 0, at, :], zp[y, 1, at, :]]
                acc = list(acc)
                for k, v in zip(terms, values):
                    for i in range(nb):
                        acc[i] = acc[i] + spread(cf, (k, i), j * ly + y) * v
                return tuple(acc)
            acc = lax.fori_loop(0, nb, body, tuple(empty() for _ in range(nb)))
            for i in range(nb):
                loc[y, i * 8:(i + 1) * 8] = acc[i]

    def x_terms(n, y, value):
        acc = tuple(loc[y, i * 8:(i + 1) * 8] for i in range(nb))
        for side, entry in enumerate(x_sides):
            when(entry[1], lambda: x_arrived(n, side, y))
            k = entry[0]

            def body(j, acc):
                v = value(side, y, pl.ds(pl.multiple_of(j * 8, 8), 8))
                return tuple(acc[i] + spread(cf, (k, i), j * ly + y) * v for i in range(nb))
            acc = lax.fori_loop(0, nb, body, acc)
        return acc

    for n in range(ITERS - 1):
        halos(n)
        local_rows(n, lambda y, j: vp[n, y, pl.ds(pl.multiple_of(j * 8, 8), 8), :], 1,
                   lambda y: (zr[n, 0, y], zr[n, 1, y]))
        for y in order:
            acc = x_terms(n, y, lambda side, y, at: xb[n, side, y, at, :])
            for i in range(nb):
                vp[n + 1, 1 + y, i * 8:(i + 1) * 8] = acc[i]
            send_x(n + 1, y)
            send_yz(n + 1, y)

    sums = ar_done(aa, 0)
    red0 = unpack32(sums[0:1], sums[1:2])
    sigma = jnp.broadcast_to(lane_sum(jnp.where((row < ly) & (lane == 8), red0, 0.0)), (8, 128))
    sigma = jnp.broadcast_to(jnp.sum(sigma, axis=0, keepdims=True), (8, 128)) / (8.0 * cells)
    nu = jnp.broadcast_to(lane_sum(jnp.where(lane == 9, red0, 0.0)), (8, 128))
    nu = jnp.broadcast_to(jnp.sum(nu, axis=0, keepdims=True), (8, 128)) / (8.0 * cells)
    inv = 1.0 / nu
    sig1, inv1 = sigma[0:1], inv[0:1]

    def shift1(v0, v1):
        return (v1 - sig1 * v0) * inv1

    def shift2(v0, v1, v2):
        return ((v2 - sig1 * v1) * inv1 - sig1 * shift1(v0, v1)) * inv1

    for y in range(ly):
        p1[y] = shift1(vp[0, 1 + y], vp[1, 1 + y])
        p2[1 + y] = shift2(vp[0, 1 + y], vp[1, 1 + y], vp[2, 1 + y])
    g1 = gram_end(gram(1), 16)
    g2 = gram_end(gram(2), 32)
    ar_start(ab, 1, pack32(g2) + pack16(g1) + [jnp.zeros((1, 128), F32)])

    for side in range(len(x_sides)):
        for y in range(ly):
            xg[side, y] = sig1 * xb[1, side, y] * inv1 + sig1 * shift1(xb[0, side, y], xb[1, side, y])
    halos(2)
    for h in (0, ly + 1):
        p2[h] = shift2(vp[0, h], vp[1, h], vp[2, h])
    local_rows(2, lambda y, j: p2[y, pl.ds(pl.multiple_of(j * 8, 8), 8), :], 1,
               lambda y: tuple(shift2(zr[0, s, y], zr[1, s, y], zr[2, s, y]) for s in range(2)))
    acc3 = gram_zero(3)
    for y in order:
        acc = x_terms(2, y, lambda side, y, at: (xb[2, side, y, at, :] * inv1 - xg[side, y, at, :]) * inv1)
        for i in range(nb):
            p3[y, i * 8:(i + 1) * 8] = (acc[i] - sig1 * p2[1 + y, i * 8:(i + 1) * 8]) * inv1
        acc3 = gram_row(3, y, acc3)
    ar_start(ac, 2, pack32(gram_end(acc3, 32)))

    weights, factors = [], []

    def factor(n, red):
        base = 8 * n
        unit = jnp.where(lane == base + row, 1.0, 0.0).astype(F32)
        d = jnp.where(lane < base + 8, red, 0.0)
        if n:
            rt = dot_nt(d, pad_rows(weights))
            s = pltpu.roll(d, 128 - base, 1) - dot_nt(rt, pad_rows([rt]))
            low, aug = cholesky(s, unit - rt, base, row, lane)
            weights.append(dot_nn(aug, pad_rows(weights + [unit])))
            factors.append(rt + low)
        else:
            low, aug = cholesky(d, unit, base, row, lane)
            weights.append(aug)
            factors.append(low)

    def emit(n):
        cols = [column(weights[n], c) for c in range(8 * (n + 1))]

        def body(a, c):
            for y in range(ly):
                parts = []
                for i in range(n + 1):
                    part = None
                    for s in range(8):
                        t = cols[i * 8 + s] * tile_row(i, y, a * 8 + s)
                        part = t if part is None else part + t
                    parts.append(part)
                q_ref[n, pl.ds(a * nr * ly + y, 8, stride=ly), :] = sum(parts[1:], parts[0])
            return c
        lax.fori_loop(0, nb, body, 0)

    factor(0, red0)
    emit(0)
    sums = ar_done(ab, 1)
    factor(1, unpack16(sums[2:3]))
    emit(1)
    factor(2, unpack32(sums[0:1], sums[1:2]))
    emit(2)

    small[8:32] = jnp.concatenate(weights, axis=0)
    small[32:40] = factors[1]
    small[40:48] = factors[2]
    small[48:56] = sigma
    small[56:64] = nu
    for n in range(ITERS):
        for side, entry in enumerate(x_sides):
            def sent():
                for y in range(ly):
                    x_copy(n, side, y).wait_send()
            when(entry[1], sent)
        for side in range(2):
            @pl.when(z_to[side])
            def _():
                for y in range(ly):
                    z_copy(n, side, y).wait_send()
            pl.when(y_to[side])(lambda: y_copy(n, side).wait_send())
    for m, buf in enumerate((aa, ab, ac)):
        ar_wait(buf, a_send.at[m])
    sums = ar_done(ac, 2)
    small[0:8] = unpack32(sums[0:1], sums[1:2])


def finish(nb, nr, ly, q_ref, p3, small, basis_hbm, hess_hbm, rest, ob, hs, sem, hsem):
    row, lane = tile_iota()
    early = [pltpu.make_async_copy(q_ref.at[n], basis_hbm.at[n], sem.at[n]) for n in range(ITERS)]
    for copy in early:
        copy.start()
    base = 8 * ITERS
    d = jnp.where(lane < base + 8, small[0:8], 0.0)
    weights = [small[8 * (n + 1):8 * (n + 2)] for n in range(ITERS)]
    rt = dot_nt(d, pad_rows(weights))
    s = pltpu.roll(d, 128 - base, 1) - dot_nt(rt, pad_rows([rt]))
    cols = [column(rt, c) for c in range(base)]
    for a in range(nb):
        for y in range(ly):
            parts = [p3[y, a * 8:(a + 1) * 8]]
            for i in range(ITERS):
                part = None
                for t in range(8):
                    u = cols[i * 8 + t] * spread(q_ref, (i,), a * nr * ly + t * ly + y)
                    part = u if part is None else part + u
                parts.append(part)
            rest[y, a * 8:(a + 1) * 8] = parts[0] - ((parts[1] + parts[2]) + parts[3])
    unit = jnp.where(lane == row, 1.0, 0.0).astype(F32)
    low, inverse = cholesky(s, unit, base, row, lane)
    cols = [column(inverse, c) for c in range(8)]
    late = []
    half = nb // 2
    for h in range(2):
        for a in range(h * half, (h + 1) * half):
            for y in range(ly):
                part = [cols[t] * spread(rest, (y,), a * 8 + t) for t in range(8)]
                total = ((part[0] + part[1]) + (part[2] + part[3])) + ((part[4] + part[5]) + (part[6] + part[7]))
                ob[pl.ds(a * nr * ly + y, 8, stride=ly), :] = total
        at = pl.ds(h * half * nr * ly, half * nr * ly)
        copy = pltpu.make_async_copy(ob.at[at], basis_hbm.at[ITERS, at], sem.at[ITERS + h])
        copy.start()
        late.append(copy)
    factors = [small[32:40], small[40:48], rt + low]
    h = dot_nn(jnp.concatenate(weights + [empty()], axis=0), pad_rows(factors))
    hr = lax.broadcasted_iota(jnp.int32, (32, 128), 0)
    hl = lax.broadcasted_iota(jnp.int32, (32, 128), 1)
    h = h * small[56:57] + jnp.where(hr == hl, small[48:49], 0.0)
    t = jnp.concatenate([h, jnp.zeros((96, 128), F32)], axis=0).T
    for i in range(ITERS + 1):
        for j in range(ITERS):
            hs[i, j] = t[8 * i:8 * i + 8, 8 * j:8 * j + 8]
    copy = pltpu.make_async_copy(hs, hess_hbm, hsem)
    copy.start()
    for c in early + late + [copy]:
        c.wait()


def shards(mesh_sizes, rhs, blocks):
    nb, nr, lx, ly, lz = rhs.shape
    assert nb == 8 and nr == 8 and lx == 1 and lz == 128 and ly <= 8
    nx, ny, nz = mesh_sizes
    ndev = nx * ny * nz
    sides = max(1, min(2, nx - 1))
    rhs2 = pltpu.with_memory_space_constraint(rhs.reshape(nb * nr * ly, lz), pltpu.HBM)
    blk2 = pltpu.with_memory_space_constraint(blocks.reshape(7, nb, nb * ly, lz), pltpu.HBM)
    dma = pltpu.SemaphoreType.DMA
    vm = lambda *s: pltpu.VMEM(s, F32)
    hbm = pl.BlockSpec(memory_space=pltpu.HBM)
    vmem = pl.BlockSpec(memory_space=pltpu.VMEM)
    q, p3, small = pl.pallas_call(
        functools.partial(krylov, mesh_sizes, nb, nr, ly, lz),
        out_shape=(
            jax.ShapeDtypeStruct((ITERS, nb * nr * ly, lz), F32),
            jax.ShapeDtypeStruct((ly, nb * 8, lz), F32),
            jax.ShapeDtypeStruct((64, lz), F32),
        ),
        in_specs=[hbm] * 2,
        out_specs=(vmem,) * 3,
        scratch_shapes=[
            vm(nb * nr * ly, lz),
            pltpu.VMEM((7, nb, nb * ly, lz), jnp.bfloat16),
            vm(7, nb, nb * ly, lz),
            vm(ITERS, ly + 2, nb * 8, lz),
            vm(ly, nb * 8, lz),
            vm(ly + 2, nb * 8, lz),
            vm(ITERS, sides, ly, nb * 8, lz),
            vm(sides, ly, nb * 8, lz),
            vm(ITERS, ly, 8, lz),
            vm(ITERS, 2, ly, 8, lz),
            vm(ly, 2, nb * 8, lz),
            vm(ly, nb * 8, lz),
            vm(ndev, 2, lz), vm(ndev, 4, lz), vm(ndev, 2, lz),
            dma((ITERS, sides, ly)), dma((ITERS, sides, ly)),
            dma((ITERS, 2)), dma((ITERS, 2)),
            dma((ITERS, 2, ly)), dma((ITERS, 2, ly)),
            dma((3,)), dma((3,)),
            dma((8,)),
            pltpu.SemaphoreType.REGULAR((2,)),
        ],
        compiler_params=pltpu.CompilerParams(collective_id=0, has_side_effects=True, vmem_limit_bytes=48 * 1024 * 1024),
    )(rhs2, blk2)
    basis, hess = pl.pallas_call(
        functools.partial(finish, nb, nr, ly),
        out_shape=(
            jax.ShapeDtypeStruct((ITERS + 1, nb * nr * ly, lz), F32),
            jax.ShapeDtypeStruct((ITERS + 1, ITERS, 8, 8), F32),
        ),
        in_specs=[vmem] * 3,
        out_specs=(hbm,) * 2,
        scratch_shapes=[
            vm(ly, nb * 8, lz),
            vm(nb * nr * ly, lz),
            vm(ITERS + 1, ITERS, 8, 8),
            dma((ITERS + 2,)),
            dma,
        ],
        compiler_params=pltpu.CompilerParams(vmem_limit_bytes=8 * 1024 * 1024),
    )(q, p3, small)
    return basis.reshape(ITERS + 1, nb, nr, lx, ly, lz), hess.transpose(0, 2, 1, 3)


def solution(mesh):
    sizes = tuple(mesh.shape[a] for a in AXES)
    return jax.shard_map(
        functools.partial(shards, sizes),
        mesh=mesh,
        in_specs=(P(None, None, "gx", "gy", "gz"), P(None, None, None, "gx", "gy", "gz")),
        out_specs=(P(None, None, None, "gx", "gy", "gz"), P()),
        check_vma=False,
    )
```

```python
import functools

import jax
import jax.numpy as jnp
from jax import lax
from jax.experimental import pallas as pl
from jax.experimental.pallas import tpu as pltpu
from jax.sharding import PartitionSpec as P

ITERS = 3
F32 = jnp.float32
HIGH = lax.Precision.HIGHEST
AXES = ("gx", "gy", "gz")
MESH = pl.DeviceIdType.MESH


def dot_nt(a, b):
    return lax.dot_general(a, b, (((1,), (1,)), ((), ())), precision=HIGH, preferred_element_type=F32)


def dot_nn(a, b):
    return lax.dot_general(a, b, (((1,), (0,)), ((), ())), precision=HIGH, preferred_element_type=F32)


def tile_iota():
    row = lax.broadcasted_iota(jnp.int32, (8, 128), 0)
    lane = lax.broadcasted_iota(jnp.int32, (8, 128), 1)
    return row, lane


def empty():
    return jnp.zeros((8, 128), F32)


def pad_rows(pieces):
    return jnp.concatenate(pieces + [empty()] * (16 - len(pieces)), axis=0)


def spread(ref, index, r):
    return jnp.broadcast_to(ref[index + (pl.ds(r, 1), slice(None))], (8, 128))


def column(m, c):
    return jnp.broadcast_to(m[:, c:c + 1], (8, 128))


def cholesky(s, aug, row, lane):
    cols = [column(s, c) for c in range(8)]
    lower = []
    for k in range(8):
        piv = jnp.broadcast_to(cols[k][k:k + 1], (8, 128))
        rs = lax.rsqrt(piv)
        rs = rs * (1.5 - 0.5 * piv * rs * rs)
        lk = jnp.where(row >= k, cols[k] * rs, 0.0)
        lower.append(lk)
        arow = jnp.broadcast_to(aug[k:k + 1], (8, 128)) * rs
        aug = jnp.where(row == k, arow, aug - jnp.where(row > k, lk, 0.0) * arow)
        for c in range(k + 1, 8):
            cols[c] = cols[c] - lk * jnp.broadcast_to(lk[c:c + 1], (8, 128))
    return lower, aug


def krylov(
    mesh_sizes, nb, nr, ly, lz,
    rhs_hbm, blk_hbm, q_ref, p3, small,
    rv, bv, cf, cz, vp, p1, p2, xb, xg, zs, zr, zp, hz, loc, aa, ab, ac,
    x_send, x_recv, y_send, y_recv, z_send, z_recv, a_send, a_recv, in_sem, known,
):
    nx, ny, nz = mesh_sizes
    ndev = nx * ny * nz
    gx, gy, gz = (lax.axis_index(a) for a in AXES)
    me = (gx * ny + gy) * nz + gz
    cells = ndev * ly * lz
    row, lane = tile_iota()
    barrier = pltpu.get_barrier_semaphore()

    in_rhs = pltpu.make_async_copy(rhs_hbm, rv, in_sem.at[0])
    in_blk = pltpu.make_async_copy(blk_hbm, bv, in_sem.at[1])
    in_rhs.start()
    in_blk.start()

    def wrapped(at, d, size):
        t = at + d
        return jnp.where(t >= size, t - size, t)

    def greet(sem, axis):
        size, at = {"gx": (nx, gx), "gy": (ny, gy), "gz": (nz, gz)}[axis]
        if size <= 8:
            for d in range(1, size):
                pl.semaphore_signal(sem, inc=1, device_id={axis: wrapped(at, d, size)}, device_id_type=MESH)
        else:
            def body(d, c):
                pl.semaphore_signal(sem, inc=1, device_id={axis: lax.rem(at + d, size)}, device_id_type=MESH)
                return c
            lax.fori_loop(1, size, body, 0)

    for axis in AXES[::-1]:
        greet(barrier, axis)

    if nx == 1:
        x_sides = []
    elif nx == 2:
        x_sides = [(1 + gx, None, 1 - gx)]
    else:
        x_sides = [(1, gx < nx - 1, gx + 1), (2, gx > 0, gx - 1)]

    def when(cond, fn):
        if cond is None:
            fn()
        else:
            pl.when(cond)(fn)

    def remote(src, dst, ssem, rsem, dev):
        return pltpu.make_async_remote_copy(
            src_ref=src, dst_ref=dst, send_sem=ssem, recv_sem=rsem, device_id=dev, device_id_type=MESH)

    def x_copy(n, side, y):
        opposite = side if nx == 2 else 1 - side
        return remote(vp.at[n, 1 + y], xb.at[n, opposite, y], x_send.at[side],
                      x_recv.at[n % 2, opposite, y], {"gx": x_sides[side][2]})

    def x_arrived(n, side, y):
        remote(vp.at[n, 1 + y], xb.at[n, side, y], x_send.at[side],
               x_recv.at[n % 2, side, y], {"gx": x_sides[side][2]}).wait_recv()

    def y_copy(n, side):
        if side == 0:
            return remote(vp.at[n, ly], vp.at[n, 0], y_send.at[0], y_recv.at[n % 2, 0], {"gy": gy + 1})
        return remote(vp.at[n, 1], vp.at[n, ly + 1], y_send.at[1], y_recv.at[n % 2, 1], {"gy": gy - 1})

    def z_copy(n, side, y):
        target = gz - 1 if side == 0 else gz + 1
        return remote(zs.at[n, y], zr.at[n, y, side], z_send.at[side], z_recv.at[n % 2, y], {"gz": target})

    def take(ref, sem):
        pltpu.make_async_copy(ref, ref, sem).wait()

    def z_arrived(n, y):
        pl.when(jnp.logical_and(z_from[0], z_from[1]))(lambda: take(zr.at[n, y], z_recv.at[n % 2, y]))
        pl.when(z_from[0] != z_from[1])(lambda: take(zr.at[n, y, 0], z_recv.at[n % 2, y]))

    y_to = (gy < ny - 1, gy > 0)
    y_from = (gy > 0, gy < ny - 1)
    z_to = (gz > 0, gz < nz - 1)
    z_from = (gz < nz - 1, gz > 0)

    for side in range(2):
        @pl.when(jnp.logical_not(y_from[side]))
        def _():
            for n in range(ITERS):
                vp[n, 0 if side == 0 else ly + 1] = jnp.zeros((nb * 8, 128), F32)

        @pl.when(jnp.logical_not(z_from[side]))
        def _():
            for n in range(ITERS):
                for y in range(ly):
                    zr[n, y, side] = empty()

    if nx > 2:
        for side in range(2):
            @pl.when(jnp.logical_not(x_sides[side][1]))
            def _():
                for n in range(ITERS):
                    xb[n, side] = jnp.zeros((ly, nb * 8, 128), F32)

    def send_x(n, y):
        for side, entry in enumerate(x_sides):
            when(entry[1], lambda: x_copy(n, side, y).start())

    def send_yz(n, y):
        if y == ly - 1:
            pl.when(y_to[0])(lambda: y_copy(n, 0).start())
        if y == 0:
            pl.when(y_to[1])(lambda: y_copy(n, 1).start())
        edge = empty()
        for a in range(nb):
            v = vp[n, 1 + y, a * 8:(a + 1) * 8]
            edge = jnp.where(lane // 2 == a, pltpu.roll(v, 2 * a + 1, 1), edge)
        zs[n, y] = edge
        for side in range(2):
            pl.when(z_to[side])(lambda: z_copy(n, side, y).start())

    order = [0] + ([ly - 1] if ly > 1 else []) + list(range(1, ly - 1))

    in_rhs.wait()
    for y in order:
        for a in range(nb):
            vp[0, 1 + y, a * 8:(a + 1) * 8] = rv[pl.ds(a * nr * ly + y, 8, stride=ly), :]
    pl.semaphore_wait(barrier, nx + ny + nz - 3)
    for y in order:
        send_x(0, y)
    greet(known.at[0], "gy")
    for y in order:
        send_yz(0, y)

    def shifted(i, y, v):
        zp[y, 0, i * 8:(i + 1) * 8] = pltpu.roll(v, lz - 1, 1)
        zp[y, 1, i * 8:(i + 1) * 8] = pltpu.roll(v, 1, 1)

    for y in order:
        for j in range(nb):
            shifted(j, y, vp[0, 1 + y, j * 8:(j + 1) * 8])

    in_blk.wait()

    def absolute(rows, total):
        for r in range(0, nb * ly, 8):
            total = total + jnp.abs(rows[r:r + 8])
        return total

    def convert(i, total):
        for k in (0, 1, 2, 3, 4):
            rows = bv[k, i].astype(F32)
            cf[k, i] = rows
            total = absolute(rows, total)
        plus, minus = bv[5, i].astype(F32), bv[6, i].astype(F32)
        total = absolute(minus, absolute(plus, total))
        at = lax.broadcasted_iota(jnp.int32, (nb * ly, 128), 1)
        cf[5, i] = jnp.where(at == lz - 1, 0.0, plus)
        cf[6, i] = jnp.where(at == 0, 0.0, minus)
        cz[i] = jnp.where(at == lz - 1, plus, jnp.where(at == 0, minus, 0.0))
        return total

    total_abs = lax.fori_loop(0, nb, convert, empty())
    trace = jnp.zeros((ly, 128), F32)
    for i in range(nb):
        trace = trace + cf[0, i, i * ly:(i + 1) * ly]

    def pairs(body, acc):
        return lax.fori_loop(0, nb // 2, lambda t, acc: body(2 * t + 1, body(2 * t, acc)), acc)

    views = [(vp, (0,), 1), (p1, (), 0), (p2, (), 1), (p3, (), 0)]

    def tile(i, y, a):
        ref, index, off = views[i]
        return ref[index + (off + y, pl.ds(pl.multiple_of(a * 8, 8), 8), slice(None))]

    def tile_row(i, y, r):
        ref, index, off = views[i]
        return spread(ref, index + (off + y,), r)

    def gram_row(n, y, acc):
        def body(a, acc):
            p = tile(n, y, a)
            return tuple(acc[i * 8 + s] + p * tile_row(i, y, a * 8 + s)
                         for i in range(n + 1) for s in range(8))
        return pairs(body, acc)

    def gram_zero(n):
        return tuple(empty() for _ in range(8 * (n + 1)))

    def gram_end(acc, width):
        d = empty()
        for k, part in enumerate(acc):
            d = jnp.where(lane % width == k, jnp.sum(part, axis=1, keepdims=True), d)
        return d

    def gram(n):
        acc = gram_zero(n)
        for y in range(ly):
            acc = gram_row(n, y, acc)
        return acc

    def pack32(d):
        d = jnp.where(lane // 32 == row % 4, d, 0.0)
        return [jnp.sum(d[0:4], axis=0, keepdims=True), jnp.sum(d[4:8], axis=0, keepdims=True)]

    def pack16(d):
        d = jnp.where(lane // 16 == row, d, 0.0)
        return [jnp.sum(d, axis=0, keepdims=True)]

    def unpack32(t0, t1):
        z = jnp.where(row < 4, t0, t1)
        out = z
        for g in range(1, 4):
            out = jnp.where(row % 4 == g, pltpu.roll(z, 128 - 32 * g, 1), out)
        return out

    def unpack16(t):
        z = jnp.broadcast_to(t, (8, 128))
        out = z
        for g in range(1, 8):
            out = jnp.where(row == g, pltpu.roll(z, 128 - 16 * g, 1), out)
        return out

    def ends(at, size):
        return [jnp.where(2 * at < size, size - 1 - k, k) for k in range(size)]

    def ar_start(buf, m, rows):
        for r, v in enumerate(rows):
            buf[me, r:r + 1] = v
        if ndev <= 64:
            xs = [wrapped(gx, nx - 1 - d, nx) for d in range(nx)]
            ys = [wrapped(gy, (d + ny // 2) % ny, ny) for d in range(ny)]
            for z in ends(gz, nz):
                for dx in range(nx):
                    for dy in range(ny):
                        copy = remote(buf.at[me], buf.at[me], a_send.at[m], a_recv.at[m], (xs[dx], ys[dy], z))
                        own = dx == nx - 1 and (dy + ny // 2) % ny == 0
                        when(z != gz if own else None, copy.start)
        else:
            def body(d, c):
                t = lax.rem(me + d, ndev)
                remote(buf.at[me], buf.at[me], a_send.at[m], a_recv.at[m],
                       (t // (ny * nz), (t // nz) % ny, t % nz)).start()
                return c
            lax.fori_loop(1, ndev, body, 0)

    def ar_done(buf, m):
        take(buf.at[0:ndev - 1], a_recv.at[m])
        return jnp.sum(buf[...], axis=0)

    lane_sum = lambda x: jnp.sum(x, axis=1, keepdims=True)
    pl.semaphore_wait(known.at[0], ny - 1)
    greet(known.at[1], "gx")
    d0 = gram_end(gram(0), 32)
    d0 = d0 + jnp.where(lane % 32 == 8, jnp.where(row < ly, lane_sum(jnp.concatenate(
        [trace, jnp.zeros((8 - ly, 128), F32)], axis=0)), 0.0), 0.0)
    d0 = d0 + jnp.where(lane % 32 == 9, lane_sum(total_abs), 0.0)
    pl.semaphore_wait(known.at[1], nx - 1)
    ar_start(aa, 0, pack32(d0))

    def own_row(field, y):
        def body(j, acc):
            at = pl.ds(pl.multiple_of(j * 8, 8), 8)
            values = [(0, field(y, at)), (5, zp[y, 0, at, :]), (6, zp[y, 1, at, :])]
            if y < ly - 1:
                values.append((3, field(y + 1, at)))
            if y > 0:
                values.append((4, field(y - 1, at)))
            acc = list(acc)
            for k, v in values:
                for i in range(nb):
                    acc[i] = acc[i] + spread(cf, (k, i), j * ly + y) * v
            return tuple(acc)
        acc = lax.fori_loop(0, nb, body, tuple(empty() for _ in range(nb)))
        for i in range(nb):
            loc[y, i * 8:(i + 1) * 8] = acc[i]

    def edge_row(n, y, plus, minus, field):
        edge = jnp.where(lane % 2 == 1, plus, pltpu.roll(minus, 2, 1))
        for j in range(nb):
            hz[j * 8:(j + 1) * 8] = pltpu.roll(edge, lz - 2 - 2 * j, 1)

        def body(j, acc):
            at = pl.ds(pl.multiple_of(j * 8, 8), 8)
            values = [(cz, (), hz[at, :])]
            if y == ly - 1:
                values.append((cf, (3,), field(ly, at)))
            if y == 0:
                values.append((cf, (4,), field(-1, at)))
            acc = list(acc)
            for ref, index, v in values:
                for i in range(nb):
                    acc[i] = acc[i] + spread(ref, index + (i,), j * ly + y) * v
            return tuple(acc)
        acc = pairs(body, tuple(loc[y, i * 8:(i + 1) * 8] for i in range(nb)))
        for i in range(nb):
            loc[y, i * 8:(i + 1) * 8] = acc[i]

    def y_arrived(n, y):
        if y == 0:
            pl.when(y_from[0])(lambda: y_copy(n, 0).wait_recv())
        if y == ly - 1:
            pl.when(y_from[1])(lambda: y_copy(n, 1).wait_recv())

    def x_terms(n, y, value):
        acc = tuple(loc[y, i * 8:(i + 1) * 8] for i in range(nb))
        for side, entry in enumerate(x_sides):
            when(entry[1], lambda: x_arrived(n, side, y))
            k = entry[0]

            def body(j, acc):
                v = value(side, y, pl.ds(pl.multiple_of(j * 8, 8), 8))
                return tuple(acc[i] + spread(cf, (k, i), j * ly + y) * v for i in range(nb))
            acc = pairs(body, acc)
        return acc

    def rows_of(ref):
        return lambda y, at: ref[1 + y, at, :]

    for y in order:
        own_row(rows_of(vp.at[0]), y)
    for n in range(ITERS - 1):
        for y in order:
            z_arrived(n, y)
            y_arrived(n, y)
            edge_row(n, y, zr[n, y, 0], zr[n, y, 1], rows_of(vp.at[n]))
            acc = x_terms(n, y, lambda side, y, at: xb[n, side, y, at, :])
            for i in range(nb):
                vp[n + 1, 1 + y, i * 8:(i + 1) * 8] = acc[i]
            send_x(n + 1, y)
            send_yz(n + 1, y)
            if n + 1 < ITERS - 1:
                for i in range(nb):
                    shifted(i, y, acc[i])
        if n + 1 < ITERS - 1:
            for y in order:
                own_row(rows_of(vp.at[n + 1]), y)

    sums = ar_done(aa, 0)
    red0 = unpack32(sums[0:1], sums[1:2])
    sigma = jnp.broadcast_to(lane_sum(jnp.where((row < ly) & (lane == 8), red0, 0.0)), (8, 128))
    sigma = jnp.broadcast_to(jnp.sum(sigma, axis=0, keepdims=True), (8, 128)) / (8.0 * cells)
    nu = jnp.broadcast_to(lane_sum(jnp.where(lane == 9, red0, 0.0)), (8, 128))
    nu = jnp.broadcast_to(jnp.sum(nu, axis=0, keepdims=True), (8, 128)) / (8.0 * cells)
    inv = 1.0 / nu
    sig1, inv1 = sigma[0:1], inv[0:1]

    def shift1(v0, v1):
        return (v1 - sig1 * v0) * inv1

    def shift2(v0, v1, v2):
        return ((v2 - sig1 * v1) * inv1 - sig1 * shift1(v0, v1)) * inv1

    for y in range(ly):
        p1[y] = shift1(vp[0, 1 + y], vp[1, 1 + y])
        p2[1 + y] = shift2(vp[0, 1 + y], vp[1, 1 + y], vp[2, 1 + y])
        for j in range(nb):
            shifted(j, y, p2[1 + y, j * 8:(j + 1) * 8])
    g1 = gram_end(gram(1), 16)
    g2 = gram_end(gram(2), 32)
    ar_start(ab, 1, pack32(g2) + pack16(g1) + [jnp.zeros((1, 128), F32)])

    for side in range(len(x_sides)):
        for y in range(ly):
            xg[side, y] = sig1 * xb[1, side, y] * inv1 + sig1 * shift1(xb[0, side, y], xb[1, side, y])
    for y in order:
        own_row(rows_of(p2), y)
    acc3 = gram_zero(3)
    for y in order:
        z_arrived(2, y)
        y_arrived(2, y)
        for h, near in ((0, 0), (ly + 1, ly - 1)):
            if y == near:
                p2[h] = shift2(vp[0, h], vp[1, h], vp[2, h])
        edge_row(2, y, *(shift2(zr[0, y, s], zr[1, y, s], zr[2, y, s]) for s in range(2)), rows_of(p2))
        acc = x_terms(2, y, lambda side, y, at: (xb[2, side, y, at, :] * inv1 - xg[side, y, at, :]) * inv1)
        for i in range(nb):
            p3[y, i * 8:(i + 1) * 8] = (acc[i] - sig1 * p2[1 + y, i * 8:(i + 1) * 8]) * inv1
        acc3 = gram_row(3, y, acc3)
    ar_start(ac, 2, pack32(gram_end(acc3, 32)))

    weights, factors = [], []

    def factor(n, red):
        base = 8 * n
        unit = jnp.where(lane == base + row, 1.0, 0.0).astype(F32)
        d = jnp.where(lane < base + 8, red, 0.0)
        if n:
            rt = dot_nt(d, pad_rows(weights))
            s = pltpu.roll(d, 128 - base, 1) - dot_nt(rt, pad_rows([rt]))
            lower, aug = cholesky(s, unit - rt, row, lane)
            weights.append(dot_nn(aug, pad_rows(weights + [unit])))
        else:
            rt = empty()
            lower, aug = cholesky(d, unit, row, lane)
            weights.append(aug)
        for k in range(8):
            rt = rt + jnp.where(lane == base + k, lower[k], 0.0)
        factors.append(rt)

    def emit(n):
        cols = [column(weights[n], c) for c in range(8 * (n + 1))]

        def body(a, c):
            for y in range(ly):
                parts = []
                for i in range(n + 1):
                    part = None
                    for s in range(8):
                        t = cols[i * 8 + s] * tile_row(i, y, a * 8 + s)
                        part = t if part is None else part + t
                    parts.append(part)
                q_ref[n, pl.ds(a * nr * ly + y, 8, stride=ly), :] = sum(parts[1:], parts[0])
            return c
        lax.fori_loop(0, nb, body, 0)

    factor(0, red0)
    emit(0)
    sums = ar_done(ab, 1)
    factor(1, unpack16(sums[2:3]))
    emit(1)
    factor(2, unpack32(sums[0:1], sums[1:2]))
    emit(2)

    h = dot_nn(jnp.concatenate(weights + [empty()], axis=0), pad_rows(factors[1:]))
    hr = lax.broadcasted_iota(jnp.int32, (32, 128), 0)
    hl = lax.broadcasted_iota(jnp.int32, (32, 128), 1)
    h = h * nu[0:1] + jnp.where(hr == hl, sigma[0:1], 0.0)
    turned = jnp.concatenate([h, weights[2] * nu] + [empty()] * 11, axis=0).T
    small[8:32] = jnp.concatenate(weights, axis=0)
    small[32:40] = pltpu.roll(turned[16:24], 96, 1)
    for i in range(ITERS + 1):
        for j in range(ITERS):
            block = turned[8 * i:8 * i + 8]
            at = 8 * (i * ITERS + j) + 40
            small[at:at + 8] = pltpu.roll(block, 128 - 8 * j, 1) if j else block
    for side, entry in enumerate(x_sides):
        when(entry[1], lambda: take(vp.at[:, 1:1 + ly], x_send.at[side]))
    for side in range(2):
        pl.when(z_to[side])(lambda: take(zs, z_send.at[side]))
        pl.when(y_to[side])(lambda: take(vp.at[:, 0], y_send.at[side]))
    for m, buf in enumerate((aa, ab, ac)):
        take(buf.at[0:ndev - 1], a_send.at[m])
    sums = ar_done(ac, 2)
    small[0:8] = unpack32(sums[0:1], sums[1:2])


def finish(nb, nr, ly, q_ref, p3, small, basis_hbm, hess_hbm, rest, ob, hs, sem):
    row, lane = tile_iota()
    for n in range(ITERS):
        pltpu.make_async_copy(q_ref.at[n], basis_hbm.at[n], sem.at[0]).start()
    base = 8 * ITERS
    d = jnp.where(lane < base + 8, small[0:8], 0.0)
    rt = dot_nt(d, pad_rows([small[8 * (n + 1):8 * (n + 2)] for n in range(ITERS)]))
    s = pltpu.roll(d, 128 - base, 1) - dot_nt(rt, pad_rows([rt]))
    cols = [column(rt, c) for c in range(base)]
    w2 = small[32:40]

    def hess_block(i, j):
        at = 8 * (i * ITERS + j) + 40
        return small[at:at + 8]

    def last(i, columns):
        out = hess_block(i, ITERS - 1)
        for r in range(8):
            out = out + jnp.where(row == r, jnp.sum(columns[r] * w2, axis=0, keepdims=True), 0.0)
        hs[i, ITERS - 1] = out[:, :8]

    for i in range(ITERS + 1):
        for j in range(ITERS - 1):
            hs[i, j] = hess_block(i, j)[:, :8]
    for i in range(ITERS):
        last(i, cols[8 * i:8 * i + 8])
    for a in range(nb):
        for y in range(ly):
            parts = [p3[y, a * 8:(a + 1) * 8]]
            for i in range(ITERS):
                part = None
                for t in range(8):
                    u = cols[i * 8 + t] * spread(q_ref, (i,), a * nr * ly + t * ly + y)
                    part = u if part is None else part + u
                parts.append(part)
            rest[y, a * 8:(a + 1) * 8] = parts[0] - ((parts[1] + parts[2]) + parts[3])
    unit = jnp.where(lane == row, 1.0, 0.0).astype(F32)
    lower, inverse = cholesky(s, unit, row, lane)
    last(ITERS, lower)
    pltpu.make_async_copy(hs, hess_hbm, sem.at[1]).start()
    cols = [column(inverse, c) for c in range(8)]
    half = nb // 2
    for h in range(2):
        for a in range(h * half, (h + 1) * half):
            for y in range(ly):
                part = [cols[t] * spread(rest, (y,), a * 8 + t) for t in range(8)]
                total = ((part[0] + part[1]) + (part[2] + part[3])) + ((part[4] + part[5]) + (part[6] + part[7]))
                ob[pl.ds(a * nr * ly + y, 8, stride=ly), :] = total
        at = pl.ds(h * half * nr * ly, half * nr * ly)
        pltpu.make_async_copy(ob.at[at], basis_hbm.at[ITERS, at], sem.at[0]).start()
    pltpu.make_async_copy(basis_hbm, basis_hbm, sem.at[0]).wait()
    pltpu.make_async_copy(hs, hess_hbm, sem.at[1]).wait()


def shards(mesh_sizes, rhs, blocks):
    nb, nr, lx, ly, lz = rhs.shape
    assert nb == 8 and nr == 8 and lx == 1 and lz == 128 and ly <= 8
    nx, ny, nz = mesh_sizes
    ndev = nx * ny * nz
    sides = max(1, min(2, nx - 1))
    rhs2 = pltpu.with_memory_space_constraint(rhs.reshape(nb * nr * ly, lz), pltpu.HBM)
    blk2 = pltpu.with_memory_space_constraint(blocks.reshape(7, nb, nb * ly, lz), pltpu.HBM)
    dma = pltpu.SemaphoreType.DMA
    vm = lambda *s: pltpu.VMEM(s, F32)
    hbm = pl.BlockSpec(memory_space=pltpu.HBM)
    vmem = pl.BlockSpec(memory_space=pltpu.VMEM)
    q, p3, small = pl.pallas_call(
        functools.partial(krylov, mesh_sizes, nb, nr, ly, lz),
        out_shape=(
            jax.ShapeDtypeStruct((ITERS, nb * nr * ly, lz), F32),
            jax.ShapeDtypeStruct((ly, nb * 8, lz), F32),
            jax.ShapeDtypeStruct((40 + 8 * ITERS * (ITERS + 1), lz), F32),
        ),
        in_specs=[hbm] * 2,
        out_specs=(vmem,) * 3,
        scratch_shapes=[
            vm(nb * nr * ly, lz),
            pltpu.VMEM((7, nb, nb * ly, lz), jnp.bfloat16),
            vm(7, nb, nb * ly, lz),
            vm(nb, nb * ly, lz),
            vm(ITERS, ly + 2, nb * 8, lz),
            vm(ly, nb * 8, lz),
            vm(ly + 2, nb * 8, lz),
            vm(ITERS, sides, ly, nb * 8, lz),
            vm(sides, ly, nb * 8, lz),
            vm(ITERS, ly, 8, lz),
            vm(ITERS, ly, 2, 8, lz),
            vm(ly, 2, nb * 8, lz),
            vm(nb * 8, lz),
            vm(ly, nb * 8, lz),
            vm(ndev, 2, lz), vm(ndev, 4, lz), vm(ndev, 2, lz),
            dma((sides,)), dma((2, sides, ly)),
            dma((2,)), dma((2, 2)),
            dma((2,)), dma((2, ly)),
            dma((3,)), dma((3,)),
            dma((2,)),
            pltpu.SemaphoreType.REGULAR((2,)),
        ],
        compiler_params=pltpu.CompilerParams(collective_id=0, has_side_effects=True, vmem_limit_bytes=48 * 1024 * 1024),
    )(rhs2, blk2)
    basis, hess = pl.pallas_call(
        functools.partial(finish, nb, nr, ly),
        out_shape=(
            jax.ShapeDtypeStruct((ITERS + 1, nb * nr * ly, lz), F32),
            jax.ShapeDtypeStruct((ITERS + 1, ITERS, 8, 8), F32),
        ),
        in_specs=[vmem] * 3,
        out_specs=(hbm,) * 2,
        scratch_shapes=[
            vm(ly, nb * 8, lz),
            vm(nb * nr * ly, lz),
            vm(ITERS + 1, ITERS, 8, 8),
            dma((2,)),
        ],
        compiler_params=pltpu.CompilerParams(vmem_limit_bytes=8 * 1024 * 1024),
    )(q, p3, small)
    return basis.reshape(ITERS + 1, nb, nr, lx, ly, lz), hess.transpose(0, 2, 1, 3)


def solution(mesh):
    sizes = tuple(mesh.shape[a] for a in AXES)
    return jax.shard_map(
        functools.partial(shards, sizes),
        mesh=mesh,
        in_specs=(P(None, None, "gx", "gy", "gz"), P(None, None, None, "gx", "gy", "gz")),
        out_specs=(P(None, None, None, "gx", "gy", "gz"), P()),
        check_vma=False,
    )
```

```python
import functools

import jax
import jax.numpy as jnp
from jax import lax
from jax.experimental import pallas as pl
from jax.experimental.pallas import tpu as pltpu
from jax.sharding import PartitionSpec as P

ITERS = 3
F32 = jnp.float32
HIGH = lax.Precision.HIGHEST
AXES = ("gx", "gy", "gz")
MESH = pl.DeviceIdType.MESH


def dot_nn(a, b):
    return lax.dot_general(a, b, (((1,), (0,)), ((), ())), precision=HIGH, preferred_element_type=F32)


def tile_iota():
    row = lax.broadcasted_iota(jnp.int32, (8, 128), 0)
    lane = lax.broadcasted_iota(jnp.int32, (8, 128), 1)
    return row, lane


def empty():
    return jnp.zeros((8, 128), F32)


def pad_rows(pieces):
    return jnp.concatenate(pieces + [empty()] * (16 - len(pieces)), axis=0)


def spread(ref, index, r):
    return jnp.broadcast_to(ref[index + (pl.ds(r, 1), slice(None))], (8, 128))


def column(m, c):
    return jnp.broadcast_to(m[:, c:c + 1], (8, 128))


def sub(v, r):
    return jnp.broadcast_to(v[r:r + 1], (8, 128))


def root(v, r):
    piv = sub(v, r)
    rs = lax.rsqrt(piv)
    return rs * (1.5 - 0.5 * piv * rs * rs)


def tree(parts):
    while len(parts) > 1:
        parts = [a + b for a, b in zip(parts[::2], parts[1::2])] + parts[len(parts) // 2 * 2:]
    return parts[0]


def cholesky(tiles, rhs, row):
    count = len(tiles)
    rhs = [list(r) for r in rhs]
    cols = [{b: tiles[b](c) for b in range(c // 8, count)} for c in range(8 * count)]
    lower = []
    for k in range(8 * count):
        kb, kr = divmod(k, 8)
        rs = root(cols[k][kb], kr)
        lk = {b: cols[k][b] * rs for b in range(kb, count)}
        lk[kb] = jnp.where(row >= kr, lk[kb], 0.0)
        lower.append(lk)
        under = jnp.where(row > kr, lk[kb], 0.0)
        for t in range(len(rhs[0])):
            arow = sub(rhs[kb][t], kr) * rs
            rhs[kb][t] = jnp.where(row == kr, arow, rhs[kb][t] - under * arow)
            for b in range(kb + 1, count):
                rhs[b][t] = rhs[b][t] - lk[b] * arow
        for c in range(k + 1, 8 * count):
            cb, cr = divmod(c, 8)
            f = sub(lk[cb], cr)
            for b in range(cb, count):
                cols[c][b] = cols[c][b] - lk[b] * f
    return lower, rhs


def krylov(
    mesh_sizes, nb, nr, ly, lz,
    rhs_hbm, blk_hbm, q_ref, p3, small,
    rv, bv, cf, cz, vp, p1, p2, xb, xg, zs, zr, zp, hz, loc, aa, rbc,
    x_send, x_recv, y_send, y_recv, z_send, z_recv, a_send, a_recv, in_sem, known,
):
    nx, ny, nz = mesh_sizes
    ndev = nx * ny * nz
    gx, gy, gz = (lax.axis_index(a) for a in AXES)
    me = (gx * ny + gy) * nz + gz
    cells = ndev * ly * lz
    row, lane = tile_iota()
    barrier = pltpu.get_barrier_semaphore()

    in_rhs = pltpu.make_async_copy(rhs_hbm, rv, in_sem.at[0])
    in_blk = pltpu.make_async_copy(blk_hbm, bv, in_sem.at[1])
    in_rhs.start()
    in_blk.start()

    def wrapped(at, d, size):
        t = at + d
        return jnp.where(t >= size, t - size, t)

    def greet(sem, axis):
        size, at = {"gx": (nx, gx), "gy": (ny, gy), "gz": (nz, gz)}[axis]
        if size <= 8:
            for d in range(1, size):
                pl.semaphore_signal(sem, inc=1, device_id={axis: wrapped(at, d, size)}, device_id_type=MESH)
        else:
            def body(d, c):
                pl.semaphore_signal(sem, inc=1, device_id={axis: lax.rem(at + d, size)}, device_id_type=MESH)
                return c
            lax.fori_loop(1, size, body, 0)

    if nx == 1:
        x_sides = []
    elif nx == 2:
        x_sides = [(1 + gx, None, 1 - gx)]
    else:
        x_sides = [(1, gx < nx - 1, gx + 1), (2, gx > 0, gx - 1)]

    def when(cond, fn):
        if cond is None:
            fn()
        else:
            pl.when(cond)(fn)

    places = {"gx": (nx, gx), "gy": (ny, gy), "gz": (nz, gz)}

    def near(sem, axes):
        for axis in axes:
            size, at = places[axis]
            for cond, target in ((at > 0, at - 1), (at < size - 1, at + 1)):
                if size > 1:
                    pl.when(cond)(lambda: pl.semaphore_signal(
                        sem, inc=1, device_id={axis: target}, device_id_type=MESH))

    def near_wait(sem, axes):
        pl.semaphore_wait(sem, sum(jnp.minimum(places[a][1], 1) + jnp.minimum(places[a][0] - 1 - places[a][1], 1)
                                   for a in axes if places[a][0] > 1))

    near(barrier, AXES[::-1])
    wave_axes = [a for a in AXES[::-1] if places[a][0] > 2]
    waves = max(nx, ny, nz) - 2 if wave_axes else 0

    def remote(src, dst, ssem, rsem, dev):
        return pltpu.make_async_remote_copy(
            src_ref=src, dst_ref=dst, send_sem=ssem, recv_sem=rsem, device_id=dev, device_id_type=MESH)

    def x_copy(n, side, y):
        opposite = side if nx == 2 else 1 - side
        return remote(vp.at[n, 1 + y], xb.at[n, opposite, y], x_send.at[side],
                      x_recv.at[n % 2, opposite, y], {"gx": x_sides[side][2]})

    def x_arrived(n, side, y):
        remote(vp.at[n, 1 + y], xb.at[n, side, y], x_send.at[side],
               x_recv.at[n % 2, side, y], {"gx": x_sides[side][2]}).wait_recv()

    def y_copy(n, side):
        if side == 0:
            return remote(vp.at[n, ly], vp.at[n, 0], y_send.at[0], y_recv.at[n % 2, 0], {"gy": gy + 1})
        return remote(vp.at[n, 1], vp.at[n, ly + 1], y_send.at[0], y_recv.at[n % 2, 1], {"gy": gy - 1})

    def z_copy(n, side, y):
        target = gz - 1 if side == 0 else gz + 1
        return remote(zs.at[n, y], zr.at[n, y, side], z_send.at[0], z_recv.at[n % 2, y], {"gz": target})

    def take(ref, sem):
        pltpu.make_async_copy(ref, ref, sem).wait()

    def z_arrived(n, y):
        pl.when(jnp.logical_and(z_from[0], z_from[1]))(lambda: take(zr.at[n, y], z_recv.at[n % 2, y]))
        pl.when(z_from[0] != z_from[1])(lambda: take(zr.at[n, y, 0], z_recv.at[n % 2, y]))

    y_to = (gy < ny - 1, gy > 0)
    y_from = (gy > 0, gy < ny - 1)
    z_to = (gz > 0, gz < nz - 1)
    z_from = (gz < nz - 1, gz > 0)

    for side in range(2):
        @pl.when(jnp.logical_not(y_from[side]))
        def _():
            for n in range(ITERS):
                vp[n, 0 if side == 0 else ly + 1] = jnp.zeros((nb * 8, 128), F32)

        @pl.when(jnp.logical_not(z_from[side]))
        def _():
            for n in range(ITERS):
                for y in range(ly):
                    zr[n, y, side] = empty()

    if nx > 2:
        for side in range(2):
            @pl.when(jnp.logical_not(x_sides[side][1]))
            def _():
                for n in range(ITERS):
                    xb[n, side] = jnp.zeros((ly, nb * 8, 128), F32)

    def send_x(n, y):
        for side, entry in enumerate(x_sides):
            when(entry[1], lambda: x_copy(n, side, y).start())

    def send_yz(n, y):
        if y == ly - 1:
            pl.when(y_to[0])(lambda: y_copy(n, 0).start())
        if y == 0:
            pl.when(y_to[1])(lambda: y_copy(n, 1).start())
        edge = empty()
        for a in range(nb):
            v = vp[n, 1 + y, a * 8:(a + 1) * 8]
            edge = jnp.where(lane // 2 == a, pltpu.roll(v, 2 * a + 1, 1), edge)
        zs[n, y] = edge
        for side in range(2):
            pl.when(z_to[side])(lambda: z_copy(n, side, y).start())

    order = [0] + ([ly - 1] if ly > 1 else []) + list(range(1, ly - 1))

    in_rhs.wait()
    for y in order:
        for a in range(nb):
            vp[0, 1 + y, a * 8:(a + 1) * 8] = rv[pl.ds(a * nr * ly + y, 8, stride=ly), :]
    near_wait(barrier, AXES)
    for y in order:
        send_x(0, y)
    if waves:
        near(known.at[0], wave_axes)
    for y in order:
        send_yz(0, y)

    def shifted(i, y, v):
        zp[y, 0, i * 8:(i + 1) * 8] = pltpu.roll(v, lz - 1, 1)
        zp[y, 1, i * 8:(i + 1) * 8] = pltpu.roll(v, 1, 1)

    for y in order:
        for j in range(nb):
            shifted(j, y, vp[0, 1 + y, j * 8:(j + 1) * 8])

    in_blk.wait()

    def absolute(rows, total):
        for r in range(0, nb * ly, 8):
            total = total + jnp.abs(rows[r:r + 8])
        return total

    def convert(i, total):
        for k in (0, 1, 2, 3, 4):
            rows = bv[k, i].astype(F32)
            cf[k, i] = rows
            total = absolute(rows, total)
        plus, minus = bv[5, i].astype(F32), bv[6, i].astype(F32)
        total = absolute(minus, absolute(plus, total))
        at = lax.broadcasted_iota(jnp.int32, (nb * ly, 128), 1)
        cf[5, i] = jnp.where(at == lz - 1, 0.0, plus)
        cf[6, i] = jnp.where(at == 0, 0.0, minus)
        cz[i] = jnp.where(at == lz - 1, plus, jnp.where(at == 0, minus, 0.0))
        return total

    total_abs = lax.fori_loop(0, nb, convert, empty())
    trace = jnp.zeros((ly, 128), F32)
    for i in range(nb):
        trace = trace + cf[0, i, i * ly:(i + 1) * ly]

    def pairs(body, acc):
        return lax.fori_loop(0, nb // 2, lambda t, acc: body(2 * t + 1, body(2 * t, acc)), acc)

    views = [(vp, (0,), 1), (p1, (), 0), (p2, (), 1), (p3, (), 0)]
    raw = [(vp, (0,), 1), (vp, (1,), 1)]

    def tile(i, y, a, fields):
        ref, index, off = fields[i]
        return ref[index + (off + y, pl.ds(pl.multiple_of(a * 8, 8), 8), slice(None))]

    def tile_row(i, y, r, fields):
        ref, index, off = fields[i]
        return spread(ref, index + (off + y,), r)

    def gram_row(n, y, acc):
        own = raw if n < 2 else views

        def body(a, acc):
            p = tile(n, y, a, own)
            return tuple(acc[i * 8 + s] + p * tile_row(i, y, a * 8 + s, own)
                         for i in range(n + 1) for s in range(8))
        return pairs(body, acc)

    def gram_zero(n):
        return tuple(empty() for _ in range(8 * (n + 1)))

    def gram_end(acc, first=0):
        d = empty()
        for k, part in enumerate(acc):
            d = jnp.where(lane % 32 == first + k, jnp.sum(part, axis=1, keepdims=True), d)
        return d

    def gram(n):
        acc = gram_zero(n)
        for y in range(ly):
            acc = gram_row(n, y, acc)
        return acc

    def pack32(d):
        d = jnp.where(lane // 32 == row % 4, d, 0.0)
        return [jnp.sum(d[0:4], axis=0, keepdims=True), jnp.sum(d[4:8], axis=0, keepdims=True)]

    def unpack32(sums):
        z = jnp.where(row < 4, sums[0:1], sums[1:2])
        out = z
        for g in range(1, 4):
            out = jnp.where(row % 4 == g, pltpu.roll(z, 128 - 32 * g, 1), out)
        return out

    def ends(at, size):
        return [jnp.where(2 * at < size, size - 1 - k, k) for k in range(size)]

    def ar_start(buf, m, rows):
        for r, v in enumerate(rows):
            buf[me, r:r + 1] = v
        if ndev <= 64:
            xs = [wrapped(gx, nx - 1 - d, nx) for d in range(nx)]
            ys = [wrapped(gy, (d + ny // 2) % ny, ny) for d in range(ny)]
            for z in ends(gz, nz):
                for dx in range(nx):
                    for dy in range(ny):
                        copy = remote(buf.at[me], buf.at[me], a_send.at[min(m, 1)], a_recv.at[m], (xs[dx], ys[dy], z))
                        own = dx == nx - 1 and (dy + ny // 2) % ny == 0
                        when(z != gz if own else None, copy.start)
        else:
            def body(d, c):
                t = lax.rem(me + d, ndev)
                remote(buf.at[me], buf.at[me], a_send.at[min(m, 1)], a_recv.at[m],
                       (t // (ny * nz), (t // nz) % ny, t % nz)).start()
                return c
            lax.fori_loop(1, ndev, body, 0)

    def ar_done(buf, m):
        take(buf.at[0:ndev - 1], a_recv.at[m])
        return jnp.sum(buf[...], axis=0)

    lane_sum = lambda x: jnp.sum(x, axis=1, keepdims=True)

    def own_row(field, y):
        def body(j, acc):
            at = pl.ds(pl.multiple_of(j * 8, 8), 8)
            values = [(0, field(y, at)), (5, zp[y, 0, at, :]), (6, zp[y, 1, at, :])]
            if y < ly - 1:
                values.append((3, field(y + 1, at)))
            if y > 0:
                values.append((4, field(y - 1, at)))
            acc = list(acc)
            for k, v in values:
                for i in range(nb):
                    acc[i] = acc[i] + spread(cf, (k, i), j * ly + y) * v
            return tuple(acc)
        acc = pairs(body, tuple(empty() for _ in range(nb)))
        for i in range(nb):
            loc[y, i * 8:(i + 1) * 8] = acc[i]

    def edge_row(n, y, plus, minus, field):
        for j in range(nb):
            first = pltpu.roll(minus, lz - 2 * j, 1) if j else minus
            hz[j * 8:(j + 1) * 8] = jnp.where(lane == 0, first, pltpu.roll(plus, lz - 2 - 2 * j, 1))

        def body(j, acc):
            at = pl.ds(pl.multiple_of(j * 8, 8), 8)
            values = [(cz, (), hz[at, :])]
            if y == ly - 1:
                values.append((cf, (3,), field(ly, at)))
            if y == 0:
                values.append((cf, (4,), field(-1, at)))
            acc = list(acc)
            for ref, index, v in values:
                for i in range(nb):
                    acc[i] = acc[i] + spread(ref, index + (i,), j * ly + y) * v
            return tuple(acc)
        acc = pairs(body, tuple(loc[y, i * 8:(i + 1) * 8] for i in range(nb)))
        for i in range(nb):
            loc[y, i * 8:(i + 1) * 8] = acc[i]

    def y_arrived(n, y):
        if y == 0:
            pl.when(y_from[0])(lambda: y_copy(n, 0).wait_recv())
        if y == ly - 1:
            pl.when(y_from[1])(lambda: y_copy(n, 1).wait_recv())

    def x_terms(n, y, value):
        acc = tuple(loc[y, i * 8:(i + 1) * 8] for i in range(nb))
        for side, entry in enumerate(x_sides):
            when(entry[1], lambda: x_arrived(n, side, y))
            k = entry[0]

            def body(j, acc):
                v = value(side, y, pl.ds(pl.multiple_of(j * 8, 8), 8))
                return tuple(acc[i] + spread(cf, (k, i), j * ly + y) * v for i in range(nb))
            acc = pairs(body, acc)
        return acc

    def rows_of(ref):
        return lambda y, at: ref[1 + y, at, :]

    def shift1(v0, v1):
        return (v1 - sig1 * v0) * inv1

    def shift2(v0, v1, v2):
        return ((v2 - sig1 * v1) * inv1 - sig1 * shift1(v0, v1)) * inv1

    for w in range(1, waves):
        near_wait(known.at[(w - 1) % 2], wave_axes)
        near(known.at[w % 2], wave_axes)
    for y in order:
        own_row(rows_of(vp.at[0]), y)
    if waves:
        near_wait(known.at[(waves - 1) % 2], wave_axes)
    greet(known.at[2], "gy")
    h00 = gram_end(gram(0), 16)
    traces = lane_sum(jnp.sum(trace, axis=0, keepdims=True))
    sizes = lane_sum(jnp.sum(total_abs, axis=0, keepdims=True))
    totals = jnp.where(lane[0:1] == 0, traces, jnp.where(lane[0:1] == 1, sizes, 0.0))

    def presence(step):
        if step == min(1, ly - 1):
            pl.semaphore_wait(known.at[2], ny - 1)
            greet(known.at[3], "gx")
        if step == ly - 1:
            pl.semaphore_wait(known.at[3], nx - 1)
            ar_start(aa, 0, [totals])

    for n in range(ITERS - 1):
        for step, y in enumerate(order):
            if n == 0:
                presence(step)
            z_arrived(n, y)
            y_arrived(n, y)
            edge_row(n, y, zr[n, y, 0], zr[n, y, 1], rows_of(vp.at[n]))
            acc = x_terms(n, y, lambda side, y, at: xb[n, side, y, at, :])
            for i in range(nb):
                vp[n + 1, 1 + y, i * 8:(i + 1) * 8] = acc[i]
            send_x(n + 1, y)
            send_yz(n + 1, y)
            if n + 1 < ITERS - 1:
                for i in range(nb):
                    shifted(i, y, acc[i])
        if n + 1 < ITERS - 1:
            for y in order:
                own_row(rows_of(vp.at[n + 1]), y)
            ar_start(rbc.at[0], 1, pack32(gram_end(gram(1)) + h00))

    sums = ar_done(aa, 0)
    sig1 = jnp.broadcast_to(sums[:, 0:1] / (8.0 * cells), (1, 128))
    nu1 = jnp.broadcast_to(sums[:, 1:2] / (8.0 * cells), (1, 128))
    inv1 = 1.0 / nu1
    for y in range(ly):
        p1[y] = shift1(vp[0, 1 + y], vp[1, 1 + y])

    for y in range(ly):
        p2[1 + y] = shift2(vp[0, 1 + y], vp[1, 1 + y], vp[2, 1 + y])
        for j in range(nb):
            shifted(j, y, p2[1 + y, j * 8:(j + 1) * 8])
    g2 = gram_end(gram(2))
    ar_start(rbc.at[1], 2, pack32(g2))

    for side in range(len(x_sides)):
        for y in range(ly):
            xg[side, y] = sig1 * xb[1, side, y] * inv1 + sig1 * shift1(xb[0, side, y], xb[1, side, y])
    for y in order:
        own_row(rows_of(p2), y)
    acc3 = gram_zero(3)
    for y in order:
        z_arrived(2, y)
        y_arrived(2, y)
        for h, near in ((0, 0), (ly + 1, ly - 1)):
            if y == near:
                p2[h] = shift2(vp[0, h], vp[1, h], vp[2, h])
        edge_row(2, y, *(shift2(zr[0, y, s], zr[1, y, s], zr[2, y, s]) for s in range(2)), rows_of(p2))
        acc = x_terms(2, y, lambda side, y, at: (xb[2, side, y, at, :] * inv1 - xg[side, y, at, :]) * inv1)
        for i in range(nb):
            p3[y, i * 8:(i + 1) * 8] = (acc[i] - sig1 * p2[1 + y, i * 8:(i + 1) * 8]) * inv1
        acc3 = gram_row(3, y, acc3)
    ar_start(rbc.at[2], 3, pack32(gram_end(acc3)))

    def emit(n):
        cols = [column(weights[n], c) for c in range(8 * (n + 1))]

        for a in range(nb):
            for y in range(ly):
                parts = []
                for i in range(n + 1):
                    part = None
                    for s in range(8):
                        t = cols[i * 8 + s] * tile_row(i, y, a * 8 + s, views)
                        part = t if part is None else part + t
                    parts.append(part)
                q_ref[n, pl.ds(a * nr * ly + y, 8, stride=ly), :] = sum(parts[1:], parts[0])

    h = unpack32(ar_done(rbc.at[0], 1))
    turn = jnp.concatenate([h] + [empty()] * 15, axis=0).T[0:8]
    both = pltpu.roll(h, 8, 1) + pltpu.roll(turn, 8, 1)
    first = pltpu.roll(h, 112, 1)
    g1 = jnp.where(lane < 8, (h - sig1 * first) * inv1,
                   ((h - sig1 * both) + sig1 * sig1 * pltpu.roll(h, 120, 1)) * (inv1 * inv1))
    grams = [first, g1, unpack32(ar_done(rbc.at[1], 2))]
    units = [[jnp.where(lane == 8 * n + row, 1.0, 0.0).astype(F32)] for n in range(ITERS)]
    lower, weights = cholesky([functools.partial(column, g) for g in grams], units, row)
    weights = [w[0] for w in weights]
    factors = [tree([jnp.where(lane == k, lower[k][n], 0.0) for k in range(8 * (n + 1))]) for n in range(ITERS)]
    for n in range(ITERS):
        emit(n)

    h = dot_nn(jnp.concatenate(weights + [empty()], axis=0), pad_rows(factors[1:]))
    hr = lax.broadcasted_iota(jnp.int32, (32, 128), 0)
    hl = lax.broadcasted_iota(jnp.int32, (32, 128), 1)
    h = h * nu1 + jnp.where(hr == hl, sig1, 0.0)
    turned = jnp.concatenate([h, weights[2] * nu1] + [empty()] * 11, axis=0).T
    small[8:32] = jnp.concatenate(weights + [empty()] * 13, axis=0).T[0:24]
    small[32:40] = pltpu.roll(turned[16:24], 96, 1)
    for i in range(ITERS + 1):
        for j in range(ITERS):
            block = turned[8 * i:8 * i + 8]
            at = 8 * (i * ITERS + j) + 40
            small[at:at + 8] = pltpu.roll(block, 128 - 8 * j, 1) if j else block
    for side, entry in enumerate(x_sides):
        when(entry[1], lambda: take(vp.at[:, 1:1 + ly], x_send.at[side]))
    for to, both_sides, one_side, sem in ((z_to, zr, zs, z_send), (y_to, vp.at[:, 0:2], vp.at[:, 0], y_send)):
        pl.when(jnp.logical_and(to[0], to[1]))(lambda: take(both_sides, sem.at[0]))
        pl.when(to[0] != to[1])(lambda: take(one_side, sem.at[0]))
    take(aa.at[0:ndev - 1], a_send.at[0])
    take(rbc.at[:, 0:ndev - 1], a_send.at[1])
    small[0:8] = unpack32(ar_done(rbc.at[2], 3))


def finish(nb, nr, ly, q_ref, p3, small, basis_hbm, hess_hbm, rest, ob, hs, sem):
    row, lane = tile_iota()
    for n in range(ITERS):
        pltpu.make_async_copy(q_ref.at[n], basis_hbm.at[n], sem.at[0]).start()
    base = 8 * ITERS
    d = small[0:8]
    dcols = [column(d, c) for c in range(base + 8)]
    rt = tree([dcols[c] * spread(small, (), 8 + c) for c in range(base)])
    cols = [column(rt, c) for c in range(base)]
    w2 = small[32:40]

    def hess_block(i, j):
        at = 8 * (i * ITERS + j) + 40
        return small[at:at + 8]

    def last(i, columns):
        out = hess_block(i, ITERS - 1)
        for r in range(8):
            out = out + jnp.where(row == r, jnp.sum(columns[r] * w2, axis=0, keepdims=True), 0.0)
        hs[i, ITERS - 1] = out[:, :8]

    for i in range(ITERS + 1):
        for j in range(ITERS - 1):
            hs[i, j] = hess_block(i, j)[:, :8]
    for i in range(ITERS):
        last(i, cols[8 * i:8 * i + 8])
    for a in range(nb):
        for y in range(ly):
            parts = [cols[8 * i + t] * spread(q_ref, (i,), a * nr * ly + t * ly + y) for i in range(ITERS) for t in range(8)]
            rest[y, a * 8:(a + 1) * 8] = p3[y, a * 8:(a + 1) * 8] - tree(parts)

    def gram_column(c):
        return dcols[base + c] - tree([cols[m] * sub(cols[m], c) for m in range(base)])

    unit = jnp.where(lane == row, 1.0, 0.0).astype(F32)
    lower, inverse = cholesky([gram_column], [[unit]], row)
    last(ITERS, [lk[0] for lk in lower])
    pltpu.make_async_copy(hs, hess_hbm, sem.at[1]).start()
    cols = [column(inverse[0][0], c) for c in range(8)]
    half = nb // 2
    for h in range(2):
        for a in range(h * half, (h + 1) * half):
            for y in range(ly):
                ob[pl.ds(a * nr * ly + y, 8, stride=ly), :] = tree(
                    [cols[t] * spread(rest, (y,), a * 8 + t) for t in range(8)])
        at = pl.ds(h * half * nr * ly, half * nr * ly)
        pltpu.make_async_copy(ob.at[at], basis_hbm.at[ITERS, at], sem.at[0]).start()
    pltpu.make_async_copy(basis_hbm, basis_hbm, sem.at[0]).wait()
    pltpu.make_async_copy(hs, hess_hbm, sem.at[1]).wait()


def shards(mesh_sizes, rhs, blocks):
    nb, nr, lx, ly, lz = rhs.shape
    assert nb == 8 and nr == 8 and lx == 1 and lz == 128 and ly <= 8
    nx, ny, nz = mesh_sizes
    ndev = nx * ny * nz
    sides = max(1, min(2, nx - 1))
    rhs2 = pltpu.with_memory_space_constraint(rhs.reshape(nb * nr * ly, lz), pltpu.HBM)
    blk2 = pltpu.with_memory_space_constraint(blocks.reshape(7, nb, nb * ly, lz), pltpu.HBM)
    dma = pltpu.SemaphoreType.DMA
    vm = lambda *s: pltpu.VMEM(s, F32)
    hbm = pl.BlockSpec(memory_space=pltpu.HBM)
    vmem = pl.BlockSpec(memory_space=pltpu.VMEM)
    q, p3, small = pl.pallas_call(
        functools.partial(krylov, mesh_sizes, nb, nr, ly, lz),
        out_shape=(
            jax.ShapeDtypeStruct((ITERS, nb * nr * ly, lz), F32),
            jax.ShapeDtypeStruct((ly, nb * 8, lz), F32),
            jax.ShapeDtypeStruct((40 + 8 * ITERS * (ITERS + 1), lz), F32),
        ),
        in_specs=[hbm] * 2,
        out_specs=(vmem,) * 3,
        scratch_shapes=[
            vm(nb * nr * ly, lz),
            pltpu.VMEM((7, nb, nb * ly, lz), jnp.bfloat16),
            vm(7, nb, nb * ly, lz),
            vm(nb, nb * ly, lz),
            vm(ITERS, ly + 2, nb * 8, lz),
            vm(ly, nb * 8, lz),
            vm(ly + 2, nb * 8, lz),
            vm(ITERS, sides, ly, nb * 8, lz),
            vm(sides, ly, nb * 8, lz),
            vm(ITERS, ly, 8, lz),
            vm(ITERS, ly, 2, 8, lz),
            vm(ly, 2, nb * 8, lz),
            vm(nb * 8, lz),
            vm(ly, nb * 8, lz),
            vm(ndev, 1, lz), vm(3, ndev, 2, lz),
            dma((sides,)), dma((2, sides, ly)),
            dma((1,)), dma((2, 2)),
            dma((1,)), dma((2, ly)),
            dma((2,)), dma((4,)),
            dma((2,)),
            pltpu.SemaphoreType.REGULAR((4,)),
        ],
        compiler_params=pltpu.CompilerParams(collective_id=0, has_side_effects=True, vmem_limit_bytes=48 * 1024 * 1024),
    )(rhs2, blk2)
    basis, hess = pl.pallas_call(
        functools.partial(finish, nb, nr, ly),
        out_shape=(
            jax.ShapeDtypeStruct((ITERS + 1, nb * nr * ly, lz), F32),
            jax.ShapeDtypeStruct((ITERS + 1, ITERS, 8, 8), F32),
        ),
        in_specs=[vmem] * 3,
        out_specs=(hbm,) * 2,
        scratch_shapes=[
            vm(ly, nb * 8, lz),
            vm(nb * nr * ly, lz),
            vm(ITERS + 1, ITERS, 8, 8),
            dma((2,)),
        ],
        compiler_params=pltpu.CompilerParams(vmem_limit_bytes=8 * 1024 * 1024),
    )(q, p3, small)
    return basis.reshape(ITERS + 1, nb, nr, lx, ly, lz), hess.transpose(0, 2, 1, 3)


def solution(mesh):
    sizes = tuple(mesh.shape[a] for a in AXES)
    return jax.shard_map(
        functools.partial(shards, sizes),
        mesh=mesh,
        in_specs=(P(None, None, "gx", "gy", "gz"), P(None, None, None, "gx", "gy", "gz")),
        out_specs=(P(None, None, None, "gx", "gy", "gz"), P()),
        check_vma=False,
    )
```

```python
import functools

import jax
import jax.numpy as jnp
from jax import lax
from jax.experimental import pallas as pl
from jax.experimental.pallas import tpu as pltpu
from jax.sharding import PartitionSpec as P

ITERS = 3
F32 = jnp.float32
HIGH = lax.Precision.HIGHEST
AXES = ("gx", "gy", "gz")
MESH = pl.DeviceIdType.MESH


def dot_nt(a, b):
    return lax.dot_general(a, b, (((1,), (1,)), ((), ())), precision=HIGH, preferred_element_type=F32)


def dot_nn(a, b):
    return lax.dot_general(a, b, (((1,), (0,)), ((), ())), precision=HIGH, preferred_element_type=F32)


def tile_iota():
    row = lax.broadcasted_iota(jnp.int32, (8, 128), 0)
    lane = lax.broadcasted_iota(jnp.int32, (8, 128), 1)
    return row, lane


def empty():
    return jnp.zeros((8, 128), F32)


def pad_rows(pieces):
    return jnp.concatenate(pieces + [empty()] * (16 - len(pieces)), axis=0)


def spread(ref, index, r):
    return jnp.broadcast_to(ref[index + (pl.ds(r, 1), slice(None))], (8, 128))


def column(m, c):
    return jnp.broadcast_to(m[:, c:c + 1], (8, 128))


def sub(v, r):
    return jnp.broadcast_to(v[r:r + 1], (8, 128))


def root(v, r):
    piv = sub(v, r)
    rs = lax.rsqrt(piv)
    return rs * (1.5 - 0.5 * piv * rs * rs)


def tree(parts):
    while len(parts) > 1:
        parts = [a + b for a, b in zip(parts[::2], parts[1::2])] + parts[len(parts) // 2 * 2:]
    return parts[0]


def factor_block(tile, rhs, lower, scale, solved, row):
    b = len(solved)
    size = 8 * (b + 1)
    cols = [tile(c) for c in range(size)]
    for k in range(size):
        kb, kr = divmod(k, 8)
        if kb < b:
            lk = cols[k] * scale[k]
            lower[k][b] = lk
            rhs = rhs - lk * sub(solved[kb], kr)
        else:
            rs = root(cols[k], kr)
            lk = jnp.where(row >= kr, cols[k] * rs, 0.0)
            scale.append(rs)
            lower.append({b: lk})
            arow = sub(rhs, kr) * rs
            rhs = jnp.where(row == kr, arow, rhs - jnp.where(row > kr, lk, 0.0) * arow)
        for c in range(k + 1, size):
            cb, cr = divmod(c, 8)
            cols[c] = cols[c] - lk * sub(lower[k][cb], cr)
    solved.append(rhs)


def krylov(
    mesh_sizes, nb, nr, ly, lz,
    rhs_hbm, blk_hbm, q_ref, p3, small,
    rv, bv, cf, cz, vp, p1, p2, xb, xg, zs, zr, zp, hz, loc, aa, rbc, xr, xa,
    x_send, x_recv, y_send, y_recv, z_send, z_recv, a_send, a_recv, in_sem, known,
):
    nx, ny, nz = mesh_sizes
    ndev = nx * ny * nz
    gx, gy, gz = (lax.axis_index(a) for a in AXES)
    me = (gx * ny + gy) * nz + gz
    cells = ndev * ly * lz
    row, lane = tile_iota()
    barrier = pltpu.get_barrier_semaphore()

    in_rhs = pltpu.make_async_copy(rhs_hbm, rv, in_sem.at[0])
    in_blk = pltpu.make_async_copy(blk_hbm, bv, in_sem.at[1])
    in_rhs.start()
    in_blk.start()

    def wrapped(at, d, size):
        t = at + d
        return jnp.where(t >= size, t - size, t)

    def greet(sem, axis):
        size, at = {"gx": (nx, gx), "gy": (ny, gy), "gz": (nz, gz)}[axis]
        if size <= 8:
            for d in range(1, size):
                pl.semaphore_signal(sem, inc=1, device_id={axis: wrapped(at, d, size)}, device_id_type=MESH)
        else:
            def body(d, c):
                pl.semaphore_signal(sem, inc=1, device_id={axis: lax.rem(at + d, size)}, device_id_type=MESH)
                return c
            lax.fori_loop(1, size, body, 0)

    if nx == 1:
        x_sides = []
    elif nx == 2:
        x_sides = [(1 + gx, None, 1 - gx)]
    else:
        x_sides = [(1, gx < nx - 1, gx + 1), (2, gx > 0, gx - 1)]

    def when(cond, fn):
        if cond is None:
            fn()
        else:
            pl.when(cond)(fn)

    places = {"gx": (nx, gx), "gy": (ny, gy), "gz": (nz, gz)}

    def near(sem, axes):
        for axis in axes:
            size, at = places[axis]
            for cond, target in ((at > 0, at - 1), (at < size - 1, at + 1)):
                if size > 1:
                    pl.when(cond)(lambda: pl.semaphore_signal(
                        sem, inc=1, device_id={axis: target}, device_id_type=MESH))

    def near_wait(sem, axes):
        pl.semaphore_wait(sem, sum(jnp.minimum(places[a][1], 1) + jnp.minimum(places[a][0] - 1 - places[a][1], 1)
                                   for a in axes if places[a][0] > 1))

    near(barrier, AXES[::-1])
    wave_axes = [a for a in AXES[::-1] if places[a][0] > 2]
    waves = max(nx, ny, nz) - 2 if wave_axes else 0

    def remote(src, dst, ssem, rsem, dev):
        return pltpu.make_async_remote_copy(
            src_ref=src, dst_ref=dst, send_sem=ssem, recv_sem=rsem, device_id=dev, device_id_type=MESH)

    def x_copy(n, side, y):
        opposite = side if nx == 2 else 1 - side
        return remote(vp.at[n, 1 + y], xb.at[n, opposite, y], x_send.at[side],
                      x_recv.at[n % 2, opposite, y], {"gx": x_sides[side][2]})

    def x_arrived(n, side, y):
        remote(vp.at[n, 1 + y], xb.at[n, side, y], x_send.at[side],
               x_recv.at[n % 2, side, y], {"gx": x_sides[side][2]}).wait_recv()

    def y_copy(n, side):
        if side == 0:
            return remote(vp.at[n, ly], vp.at[n, 0], y_send.at[0], y_recv.at[n % 2, 0], {"gy": gy + 1})
        return remote(vp.at[n, 1], vp.at[n, ly + 1], y_send.at[0], y_recv.at[n % 2, 1], {"gy": gy - 1})

    def z_copy(n, side, y):
        target = gz - 1 if side == 0 else gz + 1
        return remote(zs.at[n, y], zr.at[n, y, side], z_send.at[0], z_recv.at[n % 2, y], {"gz": target})

    def take(ref, sem):
        pltpu.make_async_copy(ref, ref, sem).wait()

    def z_arrived(n, y):
        pl.when(jnp.logical_and(z_from[0], z_from[1]))(lambda: take(zr.at[n, y], z_recv.at[n % 2, y]))
        pl.when(z_from[0] != z_from[1])(lambda: take(zr.at[n, y, 0], z_recv.at[n % 2, y]))

    y_to = (gy < ny - 1, gy > 0)
    y_from = (gy > 0, gy < ny - 1)
    z_to = (gz > 0, gz < nz - 1)
    z_from = (gz < nz - 1, gz > 0)

    for side in range(2):
        @pl.when(jnp.logical_not(y_from[side]))
        def _():
            for n in range(ITERS):
                vp[n, 0 if side == 0 else ly + 1] = jnp.zeros((nb * 8, 128), F32)

        @pl.when(jnp.logical_not(z_from[side]))
        def _():
            for n in range(ITERS):
                for y in range(ly):
                    zr[n, y, side] = empty()

    if nx > 2:
        for side in range(2):
            @pl.when(jnp.logical_not(x_sides[side][1]))
            def _():
                for n in range(ITERS):
                    xb[n, side] = jnp.zeros((ly, nb * 8, 128), F32)

    def send_x(n, y):
        for side, entry in enumerate(x_sides):
            when(entry[1], lambda: x_copy(n, side, y).start())

    def send_yz(n, y):
        if y == ly - 1:
            pl.when(y_to[0])(lambda: y_copy(n, 0).start())
        if y == 0:
            pl.when(y_to[1])(lambda: y_copy(n, 1).start())
        edge = empty()
        for a in range(nb):
            v = vp[n, 1 + y, a * 8:(a + 1) * 8]
            edge = jnp.where(lane // 2 == a, pltpu.roll(v, 2 * a + 1, 1), edge)
        zs[n, y] = edge
        for side in range(2):
            pl.when(z_to[side])(lambda: z_copy(n, side, y).start())

    order = [0] + ([ly - 1] if ly > 1 else []) + list(range(1, ly - 1))

    in_rhs.wait()
    for y in order:
        for a in range(nb):
            vp[0, 1 + y, a * 8:(a + 1) * 8] = rv[pl.ds(a * nr * ly + y, 8, stride=ly), :]
    near_wait(barrier, AXES)
    for y in order[:2]:
        send_x(0, y)
    if waves:
        near(known.at[0], wave_axes)
    for y in order:
        send_yz(0, y)

    def shifted(i, y, v):
        zp[y, 0, i * 8:(i + 1) * 8] = pltpu.roll(v, lz - 1, 1)
        zp[y, 1, i * 8:(i + 1) * 8] = pltpu.roll(v, 1, 1)

    for y in order:
        for j in range(nb):
            shifted(j, y, vp[0, 1 + y, j * 8:(j + 1) * 8])

    in_blk.wait()

    def absolute(rows, total):
        for r in range(0, nb * ly, 8):
            total = total + jnp.abs(rows[r:r + 8])
        return total

    def convert(i, total):
        for k in (0, 1, 2, 3, 4):
            rows = bv[k, i].astype(F32)
            cf[k, i] = rows
            total = absolute(rows, total)
        plus, minus = bv[5, i].astype(F32), bv[6, i].astype(F32)
        total = absolute(minus, absolute(plus, total))
        at = lax.broadcasted_iota(jnp.int32, (nb * ly, 128), 1)
        cf[5, i] = jnp.where(at == lz - 1, 0.0, plus)
        cf[6, i] = jnp.where(at == 0, 0.0, minus)
        cz[i] = jnp.where(at == lz - 1, plus, jnp.where(at == 0, minus, 0.0))
        return total

    total_abs = lax.fori_loop(0, nb, convert, empty())
    trace = jnp.zeros((ly, 128), F32)
    for i in range(nb):
        trace = trace + cf[0, i, i * ly:(i + 1) * ly]
    lane_sum = lambda x: jnp.sum(x, axis=1, keepdims=True)
    traces = lane_sum(jnp.sum(trace, axis=0, keepdims=True))
    sizes = lane_sum(jnp.sum(total_abs, axis=0, keepdims=True))
    totals = jnp.where(lane[0:1] == 0, traces, jnp.where(lane[0:1] == 1, sizes, 0.0))

    def cross(buf, m, part):
        buf[gx] = part
        for d in range(1, nx):
            remote(buf.at[gx], buf.at[gx], a_send.at[min(m, 1)], a_recv.at[4 + m],
                   {"gx": wrapped(gx, d, nx)}).start()

    def crossed(buf, m):
        if nx > 1:
            take(buf.at[0:nx - 1], a_recv.at[4 + m])
        return jnp.sum(buf[...], axis=0)

    if nx <= 2:
        cross(xa, 0, totals)
    for y in order[2:]:
        send_x(0, y)

    def several(count, body, acc):
        def steps(t, acc):
            for u in range(count):
                acc = body(count * t + u, acc)
            return acc
        return lax.fori_loop(0, nb // count, steps, acc)

    pairs = functools.partial(several, 2)

    views = [(vp, (0,), 1), (p1, (), 0), (p2, (), 1), (p3, (), 0)]
    raw = [(vp, (0,), 1), (vp, (1,), 1)]

    def tile(i, y, a, fields):
        ref, index, off = fields[i]
        return ref[index + (off + y, pl.ds(pl.multiple_of(a * 8, 8), 8), slice(None))]

    def tile_row(i, y, r, fields):
        ref, index, off = fields[i]
        return spread(ref, index + (off + y,), r)

    def gram_row(n, y, acc):
        own = raw if n < 2 else views

        def body(a, acc):
            p = tile(n, y, a, own)
            return tuple(acc[i * 8 + s] + p * tile_row(i, y, a * 8 + s, own)
                         for i in range(n + 1) for s in range(8))
        return several(4, body, acc)

    def gram_zero(n):
        return tuple(empty() for _ in range(8 * (n + 1)))

    def gram_end(acc, first=0):
        d = empty()
        for k, part in enumerate(acc):
            d = jnp.where(lane % 32 == first + k, jnp.sum(part, axis=1, keepdims=True), d)
        return d

    def gram(n):
        acc = gram_zero(n)
        for y in range(ly):
            acc = gram_row(n, y, acc)
        return acc

    def pack32(d):
        d = jnp.where(lane // 32 == row % 4, d, 0.0)
        return [jnp.sum(d[0:4], axis=0, keepdims=True), jnp.sum(d[4:8], axis=0, keepdims=True)]

    def unpack32(sums):
        z = jnp.where(row < 4, sums[0:1], sums[1:2])
        out = z
        for g in range(1, 4):
            out = jnp.where(row % 4 == g, pltpu.roll(z, 128 - 32 * g, 1), out)
        return out

    def ends(at, size):
        return [jnp.where(2 * at < size, size - 1 - k, k) for k in range(size)]

    def ar_start(buf, m, rows, plane=False):
        mine = gy * nz + gz if plane else me
        for r, v in enumerate(rows):
            buf[mine, r:r + 1] = v

        def to(device):
            return remote(buf.at[mine], buf.at[mine], a_send.at[min(m, 1)], a_recv.at[m], device)

        if ndev <= 64:
            xs = [wrapped(gx, nx - 1 - d, nx) for d in range(nx)]
            ys = [wrapped(gy, (d + ny // 2) % ny, ny) for d in range(ny)]
            for z in ends(gz, nz):
                for dx in range(nx - 1 if plane else 0, nx):
                    for dy in range(ny):
                        own = dx == nx - 1 and (dy + ny // 2) % ny == 0
                        when(z != gz if own else None, to((xs[dx], ys[dy], z)).start)
        else:
            count = ny * nz if plane else ndev

            def body(d, c):
                t = lax.rem(mine + d, count)
                to((gx if plane else t // (ny * nz), (t // nz) % ny, t % nz)).start()
                return c
            lax.fori_loop(1, count, body, 0)

    def ar_done(buf, m, count=ndev):
        take(buf.at[0:count - 1], a_recv.at[m])
        return jnp.sum(buf[0:count], axis=0)

    sum_r, sum_b, sum_c = (rbc.at[k * ndev:(k + 1) * ndev] for k in range(3))

    def own_row(field, y):
        def body(j, acc):
            at = pl.ds(pl.multiple_of(j * 8, 8), 8)
            values = [(0, field(y, at)), (5, zp[y, 0, at, :]), (6, zp[y, 1, at, :])]
            if y < ly - 1:
                values.append((3, field(y + 1, at)))
            if y > 0:
                values.append((4, field(y - 1, at)))
            acc = list(acc)
            for k, v in values:
                for i in range(nb):
                    acc[i] = acc[i] + spread(cf, (k, i), j * ly + y) * v
            return tuple(acc)
        acc = several(4, body, tuple(empty() for _ in range(nb)))
        for i in range(nb):
            loc[y, i * 8:(i + 1) * 8] = acc[i]

    def edge_cells(y, plus, minus):
        for j in range(nb):
            first = pltpu.roll(minus, lz - 2 * j, 1) if j else minus
            hz[y, j * 8:(j + 1) * 8] = jnp.where(lane == 0, first, pltpu.roll(plus, lz - 2 - 2 * j, 1))

    def edge_row(y, field):
        def body(j, acc):
            at = pl.ds(pl.multiple_of(j * 8, 8), 8)
            values = [(cz, (), hz[y, at, :])]
            if y == ly - 1:
                values.append((cf, (3,), field(ly, at)))
            if y == 0:
                values.append((cf, (4,), field(-1, at)))
            acc = list(acc)
            for ref, index, v in values:
                for i in range(nb):
                    acc[i] = acc[i] + spread(ref, index + (i,), j * ly + y) * v
            return tuple(acc)
        acc = pairs(body, tuple(loc[y, i * 8:(i + 1) * 8] for i in range(nb)))
        for i in range(nb):
            loc[y, i * 8:(i + 1) * 8] = acc[i]

    def y_arrived(n, y):
        if y == 0:
            pl.when(y_from[0])(lambda: y_copy(n, 0).wait_recv())
        if y == ly - 1:
            pl.when(y_from[1])(lambda: y_copy(n, 1).wait_recv())

    def x_terms(n, y, value):
        acc = tuple(loc[y, i * 8:(i + 1) * 8] for i in range(nb))
        for side, entry in enumerate(x_sides):
            when(entry[1], lambda: x_arrived(n, side, y))
            k = entry[0]

            def body(j, acc):
                v = value(side, y, pl.ds(pl.multiple_of(j * 8, 8), 8))
                return tuple(acc[i] + spread(cf, (k, i), j * ly + y) * v for i in range(nb))
            acc = pairs(body, acc)
        return acc

    def rows_of(ref):
        return lambda y, at: ref[1 + y, at, :]

    def shift1(v0, v1):
        return (v1 - sig1 * v0) * inv1

    def shift2(v0, v1, v2):
        return ((v2 - sig1 * v1) * inv1 - sig1 * shift1(v0, v1)) * inv1

    for w in range(1, waves):
        near_wait(known.at[(w - 1) % 2], wave_axes)
        near(known.at[w % 2], wave_axes)
    for y in order:
        own_row(rows_of(vp.at[0]), y)
    if waves:
        near_wait(known.at[(waves - 1) % 2], wave_axes)
    if nx > 2:
        cross(xa, 0, totals)
    greet(known.at[2], "gy")
    h00 = gram_end(gram(0), 16)
    def start_totals():
        pl.semaphore_wait(known.at[2], ny - 1)
        greet(known.at[3], "gx")
        ar_start(aa, 0, [crossed(xa, 0)], plane=True)

    for n in range(ITERS - 1):
        for step, y in enumerate(order):
            if n == 0 and step == min(2, ly - 1):
                start_totals()
            z_arrived(n, y)
            y_arrived(n, y)
            edge_cells(y, zr[n, y, 0], zr[n, y, 1])
            edge_row(y, rows_of(vp.at[n]))
            acc = x_terms(n, y, lambda side, y, at: xb[n, side, y, at, :])
            for i in range(nb):
                vp[n + 1, 1 + y, i * 8:(i + 1) * 8] = acc[i]
            send_x(n + 1, y)
            send_yz(n + 1, y)
            if n + 1 < ITERS - 1:
                for i in range(nb):
                    shifted(i, y, acc[i])
        if n + 1 < ITERS - 1:
            for y in order:
                own_row(rows_of(vp.at[n + 1]), y)
            cross(xr, 1, jnp.concatenate(pack32(gram_end(gram(1)) + h00), axis=0))

    sums = ar_done(aa, 0, ny * nz)
    sig1 = jnp.broadcast_to(sums[:, 0:1] / (8.0 * cells), (1, 128))
    nu1 = jnp.broadcast_to(sums[:, 1:2] / (8.0 * cells), (1, 128))
    inv1 = 1.0 / nu1
    for y in range(ly):
        p1[y] = shift1(vp[0, 1 + y], vp[1, 1 + y])

    for y in range(ly):
        p2[1 + y] = shift2(vp[0, 1 + y], vp[1, 1 + y], vp[2, 1 + y])
        for j in range(nb):
            shifted(j, y, p2[1 + y, j * 8:(j + 1) * 8])
    g2 = gram_end(gram(2))
    pl.semaphore_wait(known.at[3], nx - 1)
    ar_start(sum_b, 2, pack32(g2))
    pair = crossed(xr, 1)
    ar_start(sum_r, 1, [pair[0:1], pair[1:2]], plane=True)

    for side in range(len(x_sides)):
        for y in range(ly):
            xg[side, y] = sig1 * xb[1, side, y] * inv1 + sig1 * shift1(xb[0, side, y], xb[1, side, y])
    for y in order:
        own_row(rows_of(p2), y)
    acc3 = gram_zero(3)
    for group in (order[:-1], order[-1:]):
        for y in group:
            z_arrived(2, y)
            y_arrived(2, y)
        for y in group:
            for h, beside in ((0, 0), (ly + 1, ly - 1)):
                if y == beside:
                    p2[h] = shift2(vp[0, h], vp[1, h], vp[2, h])
            edge_cells(y, *(shift2(zr[0, y, s], zr[1, y, s], zr[2, y, s]) for s in range(2)))
        for y in group:
            edge_row(y, rows_of(p2))
        for y in group:
            acc = x_terms(2, y, lambda side, y, at: (xb[2, side, y, at, :] * inv1 - xg[side, y, at, :]) * inv1)
            for i in range(nb):
                p3[y, i * 8:(i + 1) * 8] = (acc[i] - sig1 * p2[1 + y, i * 8:(i + 1) * 8]) * inv1
            acc3 = gram_row(3, y, acc3)
    ar_start(sum_c, 3, pack32(gram_end(acc3)))

    def emit(n):
        cols = [column(weights[n], c) for c in range(8 * (n + 1))]

        for a in range(nb):
            for y in range(ly):
                parts = []
                for i in range(n + 1):
                    part = None
                    for s in range(8):
                        t = cols[i * 8 + s] * tile_row(i, y, a * 8 + s, views)
                        part = t if part is None else part + t
                    parts.append(part)
                q_ref[n, pl.ds(a * nr * ly + y, 8, stride=ly), :] = sum(parts[1:], parts[0])

    h = unpack32(ar_done(sum_r, 1, ny * nz))
    turn = jnp.concatenate([h] + [empty()] * 15, axis=0).T[0:8]
    both = pltpu.roll(h, 8, 1) + pltpu.roll(turn, 8, 1)
    first = pltpu.roll(h, 112, 1)
    g1 = jnp.where(lane < 8, (h - sig1 * first) * inv1,
                   ((h - sig1 * both) + sig1 * sig1 * pltpu.roll(h, 120, 1)) * (inv1 * inv1))
    lower, scale, weights = [], [], []

    def block(n, g):
        unit = jnp.where(lane == 8 * n + row, 1.0, 0.0).astype(F32)
        factor_block(functools.partial(column, g), unit, lower, scale, weights, row)
        emit(n)

    block(0, first)
    block(1, g1)
    block(2, unpack32(ar_done(sum_b, 2)))
    factors = [tree([jnp.where(lane == k, lower[k][n], 0.0) for k in range(8 * (n + 1))]) for n in range(ITERS)]

    h = dot_nn(jnp.concatenate(weights + [empty()], axis=0), pad_rows(factors[1:]))
    hr = lax.broadcasted_iota(jnp.int32, (32, 128), 0)
    hl = lax.broadcasted_iota(jnp.int32, (32, 128), 1)
    h = h * nu1 + jnp.where(hr == hl, sig1, 0.0)
    turned = jnp.concatenate([h, weights[2] * nu1] + [empty()] * 11, axis=0).T
    small[8:32] = jnp.concatenate(weights, axis=0)
    small[32:40] = pltpu.roll(turned[16:24], 96, 1)
    for i in range(ITERS + 1):
        for j in range(ITERS):
            block = turned[8 * i:8 * i + 8]
            at = 8 * (i * ITERS + j) + 40
            small[at:at + 8] = pltpu.roll(block, 128 - 8 * j, 1) if j else block
    for side, entry in enumerate(x_sides):
        when(entry[1], lambda: take(vp.at[:, 1:1 + ly], x_send.at[side]))
    for to, both_sides, one_side, sem in ((z_to, zr, zs, z_send), (y_to, vp.at[:, 0:2], vp.at[:, 0], y_send)):
        pl.when(jnp.logical_and(to[0], to[1]))(lambda: take(both_sides, sem.at[0]))
        pl.when(to[0] != to[1])(lambda: take(one_side, sem.at[0]))
    take(aa.at[0:ny * nz - 1 + nx - 1], a_send.at[0])
    take(rbc.at[0:2 * (ndev - 1) + ny * nz - 1 + nx - 1], a_send.at[1])
    small[0:8] = unpack32(ar_done(sum_c, 3))


def finish(nb, nr, ly, q_ref, p3, small, basis_hbm, hess_hbm, rest, ob, hs, sem):
    row, lane = tile_iota()
    for n in range(ITERS):
        pltpu.make_async_copy(q_ref.at[n], basis_hbm.at[n], sem.at[0]).start()
    base = 8 * ITERS
    d = small[0:8]
    d = jnp.where(lane < base + 8, d, 0.0)
    rt = dot_nt(d, pad_rows([small[8 * (n + 1):8 * (n + 2)] for n in range(ITERS)]))
    s = pltpu.roll(d, 128 - base, 1) - dot_nt(rt, pad_rows([rt]))
    cols = [column(rt, c) for c in range(base)]
    w2 = small[32:40]

    def hess_block(i, j):
        at = 8 * (i * ITERS + j) + 40
        return small[at:at + 8]

    def last(i, columns):
        out = hess_block(i, ITERS - 1)
        for r in range(8):
            out = out + jnp.where(row == r, jnp.sum(columns[r] * w2, axis=0, keepdims=True), 0.0)
        hs[i, ITERS - 1] = out[:, :8]

    for i in range(ITERS + 1):
        for j in range(ITERS - 1):
            hs[i, j] = hess_block(i, j)[:, :8]
    for i in range(ITERS):
        last(i, cols[8 * i:8 * i + 8])
    for a in range(nb):
        for y in range(ly):
            parts = [cols[8 * i + t] * spread(q_ref, (i,), a * nr * ly + t * ly + y) for i in range(ITERS) for t in range(8)]
            rest[y, a * 8:(a + 1) * 8] = p3[y, a * 8:(a + 1) * 8] - tree(parts)

    unit = jnp.where(lane == row, 1.0, 0.0).astype(F32)
    lower, inverse = [], []
    factor_block(functools.partial(column, s), unit, lower, [], inverse, row)
    last(ITERS, [lk[0] for lk in lower])
    pltpu.make_async_copy(hs, hess_hbm, sem.at[1]).start()
    cols = [column(inverse[0], c) for c in range(8)]
    half = nb // 2
    for h in range(2):
        for a in range(h * half, (h + 1) * half):
            for y in range(ly):
                ob[pl.ds(a * nr * ly + y, 8, stride=ly), :] = tree(
                    [cols[t] * spread(rest, (y,), a * 8 + t) for t in range(8)])
        at = pl.ds(h * half * nr * ly, half * nr * ly)
        pltpu.make_async_copy(ob.at[at], basis_hbm.at[ITERS, at], sem.at[0]).start()
    pltpu.make_async_copy(basis_hbm, basis_hbm, sem.at[0]).wait()
    pltpu.make_async_copy(hs, hess_hbm, sem.at[1]).wait()


def shards(mesh_sizes, rhs, blocks):
    nb, nr, lx, ly, lz = rhs.shape
    assert nb == 8 and nr == 8 and lx == 1 and lz == 128 and ly <= 8
    nx, ny, nz = mesh_sizes
    ndev = nx * ny * nz
    sides = max(1, min(2, nx - 1))
    rhs2 = pltpu.with_memory_space_constraint(rhs.reshape(nb * nr * ly, lz), pltpu.HBM)
    blk2 = pltpu.with_memory_space_constraint(blocks.reshape(7, nb, nb * ly, lz), pltpu.HBM)
    dma = pltpu.SemaphoreType.DMA
    vm = lambda *s: pltpu.VMEM(s, F32)
    hbm = pl.BlockSpec(memory_space=pltpu.HBM)
    vmem = pl.BlockSpec(memory_space=pltpu.VMEM)
    q, p3, small = pl.pallas_call(
        functools.partial(krylov, mesh_sizes, nb, nr, ly, lz),
        out_shape=(
            jax.ShapeDtypeStruct((ITERS, nb * nr * ly, lz), F32),
            jax.ShapeDtypeStruct((ly, nb * 8, lz), F32),
            jax.ShapeDtypeStruct((40 + 8 * ITERS * (ITERS + 1), lz), F32),
        ),
        in_specs=[hbm] * 2,
        out_specs=(vmem,) * 3,
        scratch_shapes=[
            vm(nb * nr * ly, lz),
            pltpu.VMEM((7, nb, nb * ly, lz), jnp.bfloat16),
            vm(7, nb, nb * ly, lz),
            vm(nb, nb * ly, lz),
            vm(ITERS, ly + 2, nb * 8, lz),
            vm(ly, nb * 8, lz),
            vm(ly + 2, nb * 8, lz),
            vm(ITERS, sides, ly, nb * 8, lz),
            vm(sides, ly, nb * 8, lz),
            vm(ITERS, ly, 8, lz),
            vm(ITERS, ly, 2, 8, lz),
            vm(ly, 2, nb * 8, lz),
            vm(ly, nb * 8, lz),
            vm(ly, nb * 8, lz),
            vm(ndev, 1, lz), vm(3 * ndev, 2, lz), vm(nx, 2, lz), vm(nx, 1, lz),
            dma((sides,)), dma((2, sides, ly)),
            dma((1,)), dma((2, 2)),
            dma((1,)), dma((2, ly)),
            dma((2,)), dma((6,)),
            dma((2,)),
            pltpu.SemaphoreType.REGULAR((4,)),
        ],
        compiler_params=pltpu.CompilerParams(collective_id=0, has_side_effects=True, vmem_limit_bytes=48 * 1024 * 1024),
    )(rhs2, blk2)
    basis, hess = pl.pallas_call(
        functools.partial(finish, nb, nr, ly),
        out_shape=(
            jax.ShapeDtypeStruct((ITERS + 1, nb * nr * ly, lz), F32),
            jax.ShapeDtypeStruct((ITERS + 1, ITERS, 8, 8), F32),
        ),
        in_specs=[vmem] * 3,
        out_specs=(hbm,) * 2,
        scratch_shapes=[
            vm(ly, nb * 8, lz),
            vm(nb * nr * ly, lz),
            vm(ITERS + 1, ITERS, 8, 8),
            dma((2,)),
        ],
        compiler_params=pltpu.CompilerParams(vmem_limit_bytes=8 * 1024 * 1024),
    )(q, p3, small)
    return basis.reshape(ITERS + 1, nb, nr, lx, ly, lz), hess.transpose(0, 2, 1, 3)


def solution(mesh):
    sizes = tuple(mesh.shape[a] for a in AXES)
    return jax.shard_map(
        functools.partial(shards, sizes),
        mesh=mesh,
        in_specs=(P(None, None, "gx", "gy", "gz"), P(None, None, None, "gx", "gy", "gz")),
        out_specs=(P(None, None, None, "gx", "gy", "gz"), P()),
        check_vma=False,
    )
```

```python
import functools

import jax
import jax.numpy as jnp
from jax import lax
from jax.experimental import pallas as pl
from jax.experimental.pallas import tpu as pltpu
from jax.sharding import PartitionSpec as P

ITERS = 3
F32 = jnp.float32
HIGH = lax.Precision.HIGHEST
AXES = ("gx", "gy", "gz")
MESH = pl.DeviceIdType.MESH


def dot_nt(a, b):
    return lax.dot_general(a, b, (((1,), (1,)), ((), ())), precision=HIGH, preferred_element_type=F32)


def dot_nn(a, b):
    return lax.dot_general(a, b, (((1,), (0,)), ((), ())), precision=HIGH, preferred_element_type=F32)


def tile_iota():
    row = lax.broadcasted_iota(jnp.int32, (8, 128), 0)
    lane = lax.broadcasted_iota(jnp.int32, (8, 128), 1)
    return row, lane


def empty():
    return jnp.zeros((8, 128), F32)


def pad_rows(pieces):
    return jnp.concatenate(pieces + [empty()] * (16 - len(pieces)), axis=0)


def spread(ref, index, r):
    return jnp.broadcast_to(ref[index + (pl.ds(r, 1), slice(None))], (8, 128))


def column(m, c):
    return jnp.broadcast_to(m[:, c:c + 1], (8, 128))


def sub(v, r):
    return jnp.broadcast_to(v[r:r + 1], (8, 128))


def root(v, r):
    piv = sub(v, r)
    rs = lax.rsqrt(piv)
    return rs * (1.5 - 0.5 * piv * rs * rs)


def tree(parts):
    while len(parts) > 1:
        parts = [a + b for a, b in zip(parts[::2], parts[1::2])] + parts[len(parts) // 2 * 2:]
    return parts[0]


def factor_block(tile, rhs, lower, scale, solved, row):
    b = len(solved)
    size = 8 * (b + 1)
    cols = [tile(c) for c in range(size)]
    for k in range(size):
        kb, kr = divmod(k, 8)
        if kb < b:
            lk = cols[k] * scale[k]
            lower[k][b] = lk
            rhs = rhs - lk * sub(solved[kb], kr)
        else:
            rs = root(cols[k], kr)
            lk = jnp.where(row >= kr, cols[k] * rs, 0.0)
            scale.append(rs)
            lower.append({b: lk})
            arow = sub(rhs, kr) * rs
            rhs = jnp.where(row == kr, arow, rhs - jnp.where(row > kr, lk, 0.0) * arow)
        for c in range(k + 1, size):
            cb, cr = divmod(c, 8)
            cols[c] = cols[c] - lk * sub(lower[k][cb], cr)
    solved.append(rhs)


def krylov(
    mesh_sizes, nb, nr, ly, lz,
    rhs_hbm, blk_hbm, q_ref, p3, small,
    rv, bv, cf, cz, vp, p1, p2, xb, xg, zs, zr, zp, hz, loc, aa, rbc, xr, xa,
    x_send, x_recv, y_send, y_recv, z_send, z_recv, a_send, a_recv, in_sem, known,
):
    nx, ny, nz = mesh_sizes
    ndev = nx * ny * nz
    gx, gy, gz = (lax.axis_index(a) for a in AXES)
    me = (gx * ny + gy) * nz + gz
    cells = ndev * ly * lz
    row, lane = tile_iota()
    barrier = pltpu.get_barrier_semaphore()

    in_rhs = pltpu.make_async_copy(rhs_hbm, rv, in_sem.at[0])
    in_blk = pltpu.make_async_copy(blk_hbm, bv, in_sem.at[1])
    in_rhs.start()
    in_blk.start()

    def wrapped(at, d, size):
        t = at + d
        return jnp.where(t >= size, t - size, t)

    def greet(sem, axis):
        size, at = {"gx": (nx, gx), "gy": (ny, gy), "gz": (nz, gz)}[axis]
        if size <= 8:
            for d in range(1, size):
                pl.semaphore_signal(sem, inc=1, device_id={axis: wrapped(at, d, size)}, device_id_type=MESH)
        else:
            def body(d, c):
                pl.semaphore_signal(sem, inc=1, device_id={axis: lax.rem(at + d, size)}, device_id_type=MESH)
                return c
            lax.fori_loop(1, size, body, 0)

    if nx == 1:
        x_sides = []
    elif nx == 2:
        x_sides = [(1 + gx, None, 1 - gx)]
    else:
        x_sides = [(1, gx < nx - 1, gx + 1), (2, gx > 0, gx - 1)]

    def when(cond, fn):
        if cond is None:
            fn()
        else:
            pl.when(cond)(fn)

    places = {"gx": (nx, gx), "gy": (ny, gy), "gz": (nz, gz)}

    def near(sem, axes):
        for axis in axes:
            size, at = places[axis]
            for cond, target in ((at > 0, at - 1), (at < size - 1, at + 1)):
                if size > 1:
                    pl.when(cond)(lambda: pl.semaphore_signal(
                        sem, inc=1, device_id={axis: target}, device_id_type=MESH))

    def near_wait(sem, axes):
        pl.semaphore_wait(sem, sum(jnp.minimum(places[a][1], 1) + jnp.minimum(places[a][0] - 1 - places[a][1], 1)
                                   for a in axes if places[a][0] > 1))

    near(barrier, AXES[::-1])
    wave_axes = [a for a in AXES[::-1] if places[a][0] > 2]
    waves = max(nx, ny, nz) - 2 if wave_axes else 0

    def remote(src, dst, ssem, rsem, dev):
        return pltpu.make_async_remote_copy(
            src_ref=src, dst_ref=dst, send_sem=ssem, recv_sem=rsem, device_id=dev, device_id_type=MESH)

    def x_copy(n, side, y):
        opposite = side if nx == 2 else 1 - side
        return remote(vp.at[n, 1 + y], xb.at[n, opposite, y], x_send.at[side],
                      x_recv.at[n % 2, opposite, y], {"gx": x_sides[side][2]})

    def x_arrived(n, side, y):
        remote(vp.at[n, 1 + y], xb.at[n, side, y], x_send.at[side],
               x_recv.at[n % 2, side, y], {"gx": x_sides[side][2]}).wait_recv()

    def y_copy(n, side):
        if side == 0:
            return remote(vp.at[n, ly], vp.at[n, 0], y_send.at[0], y_recv.at[n % 2, 0], {"gy": gy + 1})
        return remote(vp.at[n, 1], vp.at[n, ly + 1], y_send.at[0], y_recv.at[n % 2, 1], {"gy": gy - 1})

    def z_copy(n, side, y):
        target = gz - 1 if side == 0 else gz + 1
        return remote(zs.at[n, y], zr.at[n, y, side], z_send.at[0], z_recv.at[n % 2, y], {"gz": target})

    def take(ref, sem):
        pltpu.make_async_copy(ref, ref, sem).wait()

    def z_arrived(n, y):
        pl.when(jnp.logical_and(z_from[0], z_from[1]))(lambda: take(zr.at[n, y], z_recv.at[n % 2, y]))
        pl.when(z_from[0] != z_from[1])(lambda: take(zr.at[n, y, 0], z_recv.at[n % 2, y]))

    y_to = (gy < ny - 1, gy > 0)
    y_from = (gy > 0, gy < ny - 1)
    z_to = (gz > 0, gz < nz - 1)
    z_from = (gz < nz - 1, gz > 0)

    for side in range(2):
        @pl.when(jnp.logical_not(y_from[side]))
        def _():
            for n in range(ITERS):
                vp[n, 0 if side == 0 else ly + 1] = jnp.zeros((nb * 8, 128), F32)

        @pl.when(jnp.logical_not(z_from[side]))
        def _():
            for n in range(ITERS):
                for y in range(ly):
                    zr[n, y, side] = empty()

    if nx > 2:
        for side in range(2):
            @pl.when(jnp.logical_not(x_sides[side][1]))
            def _():
                for n in range(ITERS):
                    xb[n, side] = jnp.zeros((ly, nb * 8, 128), F32)

    def send_x(n, y):
        for side, entry in enumerate(x_sides):
            when(entry[1], lambda: x_copy(n, side, y).start())

    def send_yz(n, y):
        if y == ly - 1:
            pl.when(y_to[0])(lambda: y_copy(n, 0).start())
        if y == 0:
            pl.when(y_to[1])(lambda: y_copy(n, 1).start())
        edge = empty()
        for a in range(nb):
            v = vp[n, 1 + y, a * 8:(a + 1) * 8]
            edge = jnp.where(lane // 2 == a, pltpu.roll(v, 2 * a + 1, 1), edge)
        zs[n, y] = edge
        for side in range(2):
            pl.when(z_to[side])(lambda: z_copy(n, side, y).start())

    order = [0] + ([ly - 1] if ly > 1 else []) + list(range(1, ly - 1))

    in_rhs.wait()
    for y in order:
        for a in range(nb):
            vp[0, 1 + y, a * 8:(a + 1) * 8] = rv[pl.ds(a * nr * ly + y, 8, stride=ly), :]
    near_wait(barrier, AXES)
    for y in order[:2]:
        send_x(0, y)
    if waves:
        near(known.at[0], wave_axes)
    for y in order:
        send_yz(0, y)

    def shifted(i, y, v):
        zp[y, 0, i * 8:(i + 1) * 8] = pltpu.roll(v, lz - 1, 1)
        zp[y, 1, i * 8:(i + 1) * 8] = pltpu.roll(v, 1, 1)

    for y in order:
        for j in range(nb):
            shifted(j, y, vp[0, 1 + y, j * 8:(j + 1) * 8])

    in_blk.wait()

    def absolute(rows, total):
        for r in range(0, nb * ly, 8):
            total = total + jnp.abs(rows[r:r + 8])
        return total

    def convert(i, total):
        for k in (0, 1, 2, 3, 4):
            rows = bv[k, i].astype(F32)
            cf[k, i] = rows
            total = absolute(rows, total)
        plus, minus = bv[5, i].astype(F32), bv[6, i].astype(F32)
        total = absolute(minus, absolute(plus, total))
        at = lax.broadcasted_iota(jnp.int32, (nb * ly, 128), 1)
        cf[5, i] = jnp.where(at == lz - 1, 0.0, plus)
        cf[6, i] = jnp.where(at == 0, 0.0, minus)
        cz[i] = jnp.where(at == lz - 1, plus, jnp.where(at == 0, minus, 0.0))
        return total

    total_abs = lax.fori_loop(0, nb, convert, empty())
    trace = jnp.zeros((ly, 128), F32)
    for i in range(nb):
        trace = trace + cf[0, i, i * ly:(i + 1) * ly]
    lane_sum = lambda x: jnp.sum(x, axis=1, keepdims=True)
    traces = lane_sum(jnp.sum(trace, axis=0, keepdims=True))
    sizes = lane_sum(jnp.sum(total_abs, axis=0, keepdims=True))
    totals = jnp.where(lane[0:1] == 0, traces, jnp.where(lane[0:1] == 1, sizes, 0.0))

    def cross(buf, m, part):
        buf[gx] = part
        for d in range(1, nx):
            remote(buf.at[gx], buf.at[gx], a_send.at[min(m, 1)], a_recv.at[4 + m],
                   {"gx": wrapped(gx, d, nx)}).start()

    def crossed(buf, m):
        if nx > 1:
            take(buf.at[0:nx - 1], a_recv.at[4 + m])
        return jnp.sum(buf[...], axis=0)

    if nx <= 2:
        cross(xa, 0, totals)
    for y in order[2:]:
        send_x(0, y)

    def several(count, body, acc):
        def steps(t, acc):
            for u in range(count):
                acc = body(count * t + u, acc)
            return acc
        return lax.fori_loop(0, nb // count, steps, acc)

    pairs = functools.partial(several, 2)

    views = [(vp, (0,), 1), (p1, (), 0), (p2, (), 1), (p3, (), 0)]
    raw = [(vp, (0,), 1), (vp, (1,), 1)]

    def tile(i, y, a, fields):
        ref, index, off = fields[i]
        return ref[index + (off + y, pl.ds(pl.multiple_of(a * 8, 8), 8), slice(None))]

    def tile_row(i, y, r, fields):
        ref, index, off = fields[i]
        return spread(ref, index + (off + y,), r)

    def gram_row(n, y, acc):
        own = raw if n < 2 else views

        def body(a, acc):
            p = tile(n, y, a, own)
            return tuple(acc[i * 8 + s] + p * tile_row(i, y, a * 8 + s, own)
                         for i in range(n + 1) for s in range(8))
        return several(4, body, acc)

    def gram_zero(n):
        return tuple(empty() for _ in range(8 * (n + 1)))

    def gram_end(acc, first=0):
        d = empty()
        for k, part in enumerate(acc):
            d = jnp.where(lane % 32 == first + k, jnp.sum(part, axis=1, keepdims=True), d)
        return d

    def gram(n):
        acc = gram_zero(n)
        for y in range(ly):
            acc = gram_row(n, y, acc)
        return acc

    def pack32(d):
        d = jnp.where(lane // 32 == row % 4, d, 0.0)
        return [jnp.sum(d[0:4], axis=0, keepdims=True), jnp.sum(d[4:8], axis=0, keepdims=True)]

    def unpack32(sums):
        z = jnp.where(row < 4, sums[0:1], sums[1:2])
        out = z
        for g in range(1, 4):
            out = jnp.where(row % 4 == g, pltpu.roll(z, 128 - 32 * g, 1), out)
        return out

    def ends(at, size):
        return [jnp.where(2 * at < size, size - 1 - k, k) for k in range(size)]

    def ar_start(buf, m, rows, plane=False):
        mine = gy * nz + gz if plane else me
        for r, v in enumerate(rows):
            buf[mine, r:r + 1] = v

        def to(device):
            return remote(buf.at[mine], buf.at[mine], a_send.at[min(m, 1)], a_recv.at[m], device)

        if ndev <= 64:
            xs = [wrapped(gx, nx - 1 - d, nx) for d in range(nx)]
            ys = [wrapped(gy, (d + ny // 2) % ny, ny) for d in range(ny)]
            for z in ends(gz, nz):
                for dx in range(nx - 1 if plane else 0, nx):
                    for dy in range(ny):
                        own = dx == nx - 1 and (dy + ny // 2) % ny == 0
                        when(z != gz if own else None, to((xs[dx], ys[dy], z)).start)
        else:
            count = ny * nz if plane else ndev

            def body(d, c):
                t = lax.rem(mine + d, count)
                to((gx if plane else t // (ny * nz), (t // nz) % ny, t % nz)).start()
                return c
            lax.fori_loop(1, count, body, 0)

    def ar_done(buf, m, count=ndev):
        take(buf.at[0:count - 1], a_recv.at[m])
        return jnp.sum(buf[0:count], axis=0)

    sum_r, sum_b, sum_c = (rbc.at[k * ndev:(k + 1) * ndev] for k in range(3))

    def own_row(field, y):
        def body(j, acc):
            at = pl.ds(pl.multiple_of(j * 8, 8), 8)
            values = [(0, field(y, at)), (5, zp[y, 0, at, :]), (6, zp[y, 1, at, :])]
            if y < ly - 1:
                values.append((3, field(y + 1, at)))
            if y > 0:
                values.append((4, field(y - 1, at)))
            acc = list(acc)
            for k, v in values:
                for i in range(nb):
                    acc[i] = acc[i] + spread(cf, (k, i), j * ly + y) * v
            return tuple(acc)
        acc = several(4, body, tuple(empty() for _ in range(nb)))
        for i in range(nb):
            loc[y, i * 8:(i + 1) * 8] = acc[i]

    def edge_cells(y, plus, minus):
        for j in range(nb):
            first = pltpu.roll(minus, lz - 2 * j, 1) if j else minus
            hz[y, j * 8:(j + 1) * 8] = jnp.where(lane == 0, first, pltpu.roll(plus, lz - 2 - 2 * j, 1))

    def edge_row(y, field):
        def body(j, acc):
            at = pl.ds(pl.multiple_of(j * 8, 8), 8)
            values = [(cz, (), hz[y, at, :])]
            if y == ly - 1:
                values.append((cf, (3,), field(ly, at)))
            if y == 0:
                values.append((cf, (4,), field(-1, at)))
            acc = list(acc)
            for ref, index, v in values:
                for i in range(nb):
                    acc[i] = acc[i] + spread(ref, index + (i,), j * ly + y) * v
            return tuple(acc)
        acc = pairs(body, tuple(loc[y, i * 8:(i + 1) * 8] for i in range(nb)))
        for i in range(nb):
            loc[y, i * 8:(i + 1) * 8] = acc[i]

    def y_arrived(n, y):
        if y == 0:
            pl.when(y_from[0])(lambda: y_copy(n, 0).wait_recv())
        if y == ly - 1:
            pl.when(y_from[1])(lambda: y_copy(n, 1).wait_recv())

    def x_terms(n, y, value):
        acc = tuple(loc[y, i * 8:(i + 1) * 8] for i in range(nb))
        for side, entry in enumerate(x_sides):
            when(entry[1], lambda: x_arrived(n, side, y))
            k = entry[0]

            def body(j, acc):
                v = value(side, y, pl.ds(pl.multiple_of(j * 8, 8), 8))
                return tuple(acc[i] + spread(cf, (k, i), j * ly + y) * v for i in range(nb))
            acc = pairs(body, acc)
        return acc

    def rows_of(ref):
        return lambda y, at: ref[1 + y, at, :]

    def shift1(v0, v1):
        return (v1 - sig1 * v0) * inv1

    def shift2(v0, v1, v2):
        return ((v2 - sig1 * v1) * inv1 - sig1 * shift1(v0, v1)) * inv1

    for w in range(1, waves):
        near_wait(known.at[(w - 1) % 2], wave_axes)
        near(known.at[w % 2], wave_axes)
    for y in order:
        own_row(rows_of(vp.at[0]), y)
    if waves:
        near_wait(known.at[(waves - 1) % 2], wave_axes)
    if nx > 2:
        cross(xa, 0, totals)
    greet(known.at[2], "gy")
    h00 = gram_end(gram(0), 16)
    def start_totals():
        pl.semaphore_wait(known.at[2], ny - 1)
        greet(known.at[3], "gx")
        ar_start(aa, 0, [crossed(xa, 0)], plane=True)

    for n in range(ITERS - 1):
        for step, y in enumerate(order):
            if n == 0 and step == min(2, ly - 1):
                start_totals()
            z_arrived(n, y)
            y_arrived(n, y)
            edge_cells(y, zr[n, y, 0], zr[n, y, 1])
            edge_row(y, rows_of(vp.at[n]))
            acc = x_terms(n, y, lambda side, y, at: xb[n, side, y, at, :])
            for i in range(nb):
                vp[n + 1, 1 + y, i * 8:(i + 1) * 8] = acc[i]
            send_x(n + 1, y)
            send_yz(n + 1, y)
            if n + 1 < ITERS - 1:
                for i in range(nb):
                    shifted(i, y, acc[i])
        if n + 1 < ITERS - 1:
            for y in order:
                own_row(rows_of(vp.at[n + 1]), y)
            cross(xr, 1, jnp.concatenate(pack32(gram_end(gram(1)) + h00), axis=0))

    sums = ar_done(aa, 0, ny * nz)
    sig1 = jnp.broadcast_to(sums[:, 0:1] / (8.0 * cells), (1, 128))
    nu1 = jnp.broadcast_to(sums[:, 1:2] / (8.0 * cells), (1, 128))
    inv1 = 1.0 / nu1
    for y in range(ly):
        p1[y] = shift1(vp[0, 1 + y], vp[1, 1 + y])

    for y in range(ly):
        p2[1 + y] = shift2(vp[0, 1 + y], vp[1, 1 + y], vp[2, 1 + y])
        for j in range(nb):
            shifted(j, y, p2[1 + y, j * 8:(j + 1) * 8])
    g2 = gram_end(gram(2))
    pl.semaphore_wait(known.at[3], nx - 1)
    ar_start(sum_b, 2, pack32(g2))
    pair = crossed(xr, 1)
    ar_start(sum_r, 1, [pair[0:1], pair[1:2]], plane=True)

    for side in range(len(x_sides)):
        for y in range(ly):
            xg[side, y] = sig1 * xb[1, side, y] * inv1 + sig1 * shift1(xb[0, side, y], xb[1, side, y])
    for y in order:
        own_row(rows_of(p2), y)
    acc3 = gram_zero(3)
    for group in (order[:-2], order[-2:-1], order[-1:]):
        for y in group:
            z_arrived(2, y)
            y_arrived(2, y)
        for y in group:
            for h, beside in ((0, 0), (ly + 1, ly - 1)):
                if y == beside:
                    p2[h] = shift2(vp[0, h], vp[1, h], vp[2, h])
            edge_cells(y, *(shift2(zr[0, y, s], zr[1, y, s], zr[2, y, s]) for s in range(2)))
        for y in group:
            edge_row(y, rows_of(p2))
        for y in group:
            acc = x_terms(2, y, lambda side, y, at: (xb[2, side, y, at, :] * inv1 - xg[side, y, at, :]) * inv1)
            for i in range(nb):
                p3[y, i * 8:(i + 1) * 8] = (acc[i] - sig1 * p2[1 + y, i * 8:(i + 1) * 8]) * inv1
            acc3 = gram_row(3, y, acc3)
    ar_start(sum_c, 3, pack32(gram_end(acc3)))

    def emit(n):
        cols = [column(weights[n], c) for c in range(8 * (n + 1))]

        for a in range(nb):
            for y in range(ly):
                parts = []
                for i in range(n + 1):
                    part = None
                    for s in range(8):
                        t = cols[i * 8 + s] * tile_row(i, y, a * 8 + s, views)
                        part = t if part is None else part + t
                    parts.append(part)
                q_ref[n, pl.ds(a * nr * ly + y, 8, stride=ly), :] = sum(parts[1:], parts[0])

    h = unpack32(ar_done(sum_r, 1, ny * nz))
    turn = jnp.concatenate([h] + [empty()] * 15, axis=0).T[0:8]
    both = pltpu.roll(h, 8, 1) + pltpu.roll(turn, 8, 1)
    first = pltpu.roll(h, 112, 1)
    g1 = jnp.where(lane < 8, (h - sig1 * first) * inv1,
                   ((h - sig1 * both) + sig1 * sig1 * pltpu.roll(h, 120, 1)) * (inv1 * inv1))
    lower, scale, weights = [], [], []

    def block(n, g):
        unit = jnp.where(lane == 8 * n + row, 1.0, 0.0).astype(F32)
        factor_block(functools.partial(column, g), unit, lower, scale, weights, row)
        emit(n)

    block(0, first)
    block(1, g1)
    block(2, unpack32(ar_done(sum_b, 2)))
    factors = [tree([jnp.where(lane == k, lower[k][n], 0.0) for k in range(8 * (n + 1))]) for n in range(ITERS)]

    h = dot_nn(jnp.concatenate(weights + [empty()], axis=0), pad_rows(factors[1:]))
    hr = lax.broadcasted_iota(jnp.int32, (32, 128), 0)
    hl = lax.broadcasted_iota(jnp.int32, (32, 128), 1)
    h = h * nu1 + jnp.where(hr == hl, sig1, 0.0)
    turned = jnp.concatenate([h, weights[2] * nu1] + [empty()] * 11, axis=0).T
    small[8:32] = jnp.concatenate(weights, axis=0)
    small[32:40] = pltpu.roll(turned[16:24], 96, 1)
    for i in range(ITERS + 1):
        for j in range(ITERS):
            block = turned[8 * i:8 * i + 8]
            at = 8 * (i * ITERS + j) + 40
            small[at:at + 8] = pltpu.roll(block, 128 - 8 * j, 1) if j else block
    for side, entry in enumerate(x_sides):
        when(entry[1], lambda: take(vp.at[:, 1:1 + ly], x_send.at[side]))
    for to, both_sides, one_side, sem in ((z_to, zr, zs, z_send), (y_to, vp.at[:, 0:2], vp.at[:, 0], y_send)):
        pl.when(jnp.logical_and(to[0], to[1]))(lambda: take(both_sides, sem.at[0]))
        pl.when(to[0] != to[1])(lambda: take(one_side, sem.at[0]))
    take(aa.at[0:ny * nz - 1 + nx - 1], a_send.at[0])
    take(rbc.at[0:2 * (ndev - 1) + ny * nz - 1 + nx - 1], a_send.at[1])
    small[0:8] = unpack32(ar_done(sum_c, 3))


def finish(nb, nr, ly, q_ref, p3, small, basis_hbm, hess_hbm, rest, ob, hs, sem):
    row, lane = tile_iota()
    for n in range(ITERS):
        pltpu.make_async_copy(q_ref.at[n], basis_hbm.at[n], sem.at[0]).start()
    base = 8 * ITERS
    d = small[0:8]
    d = jnp.where(lane < base + 8, d, 0.0)
    rt = dot_nt(d, pad_rows([small[8 * (n + 1):8 * (n + 2)] for n in range(ITERS)]))
    s = pltpu.roll(d, 128 - base, 1) - dot_nt(rt, pad_rows([rt]))
    cols = [column(rt, c) for c in range(base)]
    w2 = small[32:40]

    def hess_block(i, j):
        at = 8 * (i * ITERS + j) + 40
        return small[at:at + 8]

    def last(i, columns):
        out = hess_block(i, ITERS - 1)
        for r in range(8):
            out = out + jnp.where(row == r, jnp.sum(columns[r] * w2, axis=0, keepdims=True), 0.0)
        hs[i, ITERS - 1] = out[:, :8]

    for i in range(ITERS + 1):
        for j in range(ITERS - 1):
            hs[i, j] = hess_block(i, j)[:, :8]
    for i in range(ITERS):
        last(i, cols[8 * i:8 * i + 8])
    for a in range(nb):
        for y in range(ly):
            parts = [cols[8 * i + t] * spread(q_ref, (i,), a * nr * ly + t * ly + y) for i in range(ITERS) for t in range(8)]
            rest[y, a * 8:(a + 1) * 8] = p3[y, a * 8:(a + 1) * 8] - tree(parts)

    unit = jnp.where(lane == row, 1.0, 0.0).astype(F32)
    lower, inverse = [], []
    factor_block(functools.partial(column, s), unit, lower, [], inverse, row)
    last(ITERS, [lk[0] for lk in lower])
    pltpu.make_async_copy(hs, hess_hbm, sem.at[1]).start()
    cols = [column(inverse[0], c) for c in range(8)]
    half = nb // 2
    for h in range(2):
        for a in range(h * half, (h + 1) * half):
            for y in range(ly):
                ob[pl.ds(a * nr * ly + y, 8, stride=ly), :] = tree(
                    [cols[t] * spread(rest, (y,), a * 8 + t) for t in range(8)])
        at = pl.ds(h * half * nr * ly, half * nr * ly)
        pltpu.make_async_copy(ob.at[at], basis_hbm.at[ITERS, at], sem.at[0]).start()
    pltpu.make_async_copy(basis_hbm, basis_hbm, sem.at[0]).wait()
    pltpu.make_async_copy(hs, hess_hbm, sem.at[1]).wait()


def shards(mesh_sizes, rhs, blocks):
    nb, nr, lx, ly, lz = rhs.shape
    assert nb == 8 and nr == 8 and lx == 1 and lz == 128 and ly <= 8
    nx, ny, nz = mesh_sizes
    ndev = nx * ny * nz
    sides = max(1, min(2, nx - 1))
    rhs2 = pltpu.with_memory_space_constraint(rhs.reshape(nb * nr * ly, lz), pltpu.HBM)
    blk2 = pltpu.with_memory_space_constraint(blocks.reshape(7, nb, nb * ly, lz), pltpu.HBM)
    dma = pltpu.SemaphoreType.DMA
    vm = lambda *s: pltpu.VMEM(s, F32)
    hbm = pl.BlockSpec(memory_space=pltpu.HBM)
    vmem = pl.BlockSpec(memory_space=pltpu.VMEM)
    q, p3, small = pl.pallas_call(
        functools.partial(krylov, mesh_sizes, nb, nr, ly, lz),
        out_shape=(
            jax.ShapeDtypeStruct((ITERS, nb * nr * ly, lz), F32),
            jax.ShapeDtypeStruct((ly, nb * 8, lz), F32),
            jax.ShapeDtypeStruct((40 + 8 * ITERS * (ITERS + 1), lz), F32),
        ),
        in_specs=[hbm] * 2,
        out_specs=(vmem,) * 3,
        scratch_shapes=[
            vm(nb * nr * ly, lz),
            pltpu.VMEM((7, nb, nb * ly, lz), jnp.bfloat16),
            vm(7, nb, nb * ly, lz),
            vm(nb, nb * ly, lz),
            vm(ITERS, ly + 2, nb * 8, lz),
            vm(ly, nb * 8, lz),
            vm(ly + 2, nb * 8, lz),
            vm(ITERS, sides, ly, nb * 8, lz),
            vm(sides, ly, nb * 8, lz),
            vm(ITERS, ly, 8, lz),
            vm(ITERS, ly, 2, 8, lz),
            vm(ly, 2, nb * 8, lz),
            vm(ly, nb * 8, lz),
            vm(ly, nb * 8, lz),
            vm(ndev, 1, lz), vm(3 * ndev, 2, lz), vm(nx, 2, lz), vm(nx, 1, lz),
            dma((sides,)), dma((2, sides, ly)),
            dma((1,)), dma((2, 2)),
            dma((1,)), dma((2, ly)),
            dma((2,)), dma((6,)),
            dma((2,)),
            pltpu.SemaphoreType.REGULAR((4,)),
        ],
        compiler_params=pltpu.CompilerParams(collective_id=0, has_side_effects=True, vmem_limit_bytes=48 * 1024 * 1024),
    )(rhs2, blk2)
    basis, hess = pl.pallas_call(
        functools.partial(finish, nb, nr, ly),
        out_shape=(
            jax.ShapeDtypeStruct((ITERS + 1, nb * nr * ly, lz), F32),
            jax.ShapeDtypeStruct((ITERS + 1, ITERS, 8, 8), F32),
        ),
        in_specs=[vmem] * 3,
        out_specs=(hbm,) * 2,
        scratch_shapes=[
            vm(ly, nb * 8, lz),
            vm(nb * nr * ly, lz),
            vm(ITERS + 1, ITERS, 8, 8),
            dma((2,)),
        ],
        compiler_params=pltpu.CompilerParams(vmem_limit_bytes=8 * 1024 * 1024),
    )(q, p3, small)
    return basis.reshape(ITERS + 1, nb, nr, lx, ly, lz), hess.transpose(0, 2, 1, 3)


def solution(mesh):
    sizes = tuple(mesh.shape[a] for a in AXES)
    return jax.shard_map(
        functools.partial(shards, sizes),
        mesh=mesh,
        in_specs=(P(None, None, "gx", "gy", "gz"), P(None, None, None, "gx", "gy", "gz")),
        out_specs=(P(None, None, None, "gx", "gy", "gz"), P()),
        check_vma=False,
    )
```
